32 devices in a mesh: dp: 1 (over z), sp: 4 (over y), tp: 8 (over x, core).
Axes of the slice: x: 4, y: 4, z: 1, core: 2. Of those that a mesh axis runs over, the one named last changes fastest.
The devices are a block of a 4x4x8 slice.
Arguments:
- hidden: bfloat16 [64, 5120], P('dp')
- new_pos: int32 [64], P('dp')
- k_self: bfloat16 [64, 256, 8, 128], P('dp', 'sp', 'tp')
- v_self: bfloat16 [64, 256, 8, 128], P('dp', 'sp', 'tp')
- k_cross: bfloat16 [64, 512, 8, 128], P('dp', None, 'tp')
- v_cross: bfloat16 [64, 512, 8, 128], P('dp', None, 'tp')
- xvalid: int32 [64, 512], P('dp')
- rowmask: int32 [64], P('dp')
- self_attn_norm: bfloat16 [5120], replicated
- self_wq: bfloat16 [5120, 4096], P(None, 'tp')
- self_wk: bfloat16 [5120, 1024], P(None, 'tp')
- self_wv: bfloat16 [5120, 1024], P(None, 'tp')
- self_wo: bfloat16 [4096, 5120], P('tp')
- self_mlp_norm: bfloat16 [5120], replicated
- self_wgate: bfloat16 [5120, 14336], P(None, 'tp')
- self_wup: bfloat16 [5120, 14336], P(None, 'tp')
- self_wdown: bfloat16 [14336, 5120], P('tp')
- cross_attn_norm: bfloat16 [5120], replicated
- cross_wq: bfloat16 [5120, 4096], P(None, 'tp')
- cross_qnorm: bfloat16 [128], replicated
- cross_wo: bfloat16 [4096, 5120], P('tp')
- cross_gates: float32 [2], replicated
- cross_mlp_norm: bfloat16 [5120], replicated
- cross_wgate: bfloat16 [5120, 14336], P(None, 'tp')
- cross_wup: bfloat16 [5120, 14336], P(None, 'tp')
- cross_wdown: bfloat16 [14336, 5120], P('tp')
Outputs:
- output 1: bfloat16 [64, 5120], P('dp')
- output 2: bfloat16 [64, 256, 8, 128], P('dp', 'sp', 'tp')
- output 3: bfloat16 [64, 256, 8, 128], P('dp', 'sp', 'tp')
All inputs are finite; a program needn't handle non-finite values.
Results may differ from the reference program's by a relative error of at most 0.0147858.
Values sent between devices are 32-bit elements.
A program may use at most 768 MiB of HBM per device.

```python
import math
import jax
import jax.numpy as jnp
from jax import lax

BATCH = 64
SEQ_LEN = 256
VIS_TOKENS = 512
HIDDEN = 5120
HEADS = 32
KV_HEADS = 8
HEAD_DIM = 128
MLP_DIM = 14336

GROUP_SIZE = HEADS // KV_HEADS
Q_WIDTH = HEADS * HEAD_DIM
KV_WIDTH = KV_HEADS * HEAD_DIM
NORM_EPS = 1e-5
ROPE_THETA = 500000.0
ROPE_FACTOR = 8.0
LOW_FREQ = 1.0
HIGH_FREQ = 4.0
ORIG_CTX = 8192.0
NEG_BIG = -1e30
KEY_SCALE = 1.6


def rope_freqs():
    inv_freq = 1.0 / (ROPE_THETA ** (jnp.arange(0, HEAD_DIM, 2).astype(jnp.float32) / HEAD_DIM))
    wavelen = 2.0 * math.pi / inv_freq
    smooth = (ORIG_CTX / wavelen - LOW_FREQ) / (HIGH_FREQ - LOW_FREQ)
    mid_freq = (1.0 - smooth) * inv_freq / ROPE_FACTOR + smooth * inv_freq
    scaled = jnp.where(wavelen > ORIG_CTX / LOW_FREQ, inv_freq / ROPE_FACTOR, mid_freq)
    return jnp.where(wavelen < ORIG_CTX / HIGH_FREQ, inv_freq, scaled)


def apply_rope(vectors, positions):
    half_dim = HEAD_DIM // 2
    angles = positions.astype(jnp.float32)[:, None] * rope_freqs()[None, :]
    cos_t = jnp.cos(angles)[:, None, :]
    sin_t = jnp.sin(angles)[:, None, :]
    first_half = vectors[..., :half_dim]
    second_half = vectors[..., half_dim:]
    return jnp.concatenate([first_half * cos_t - second_half * sin_t, second_half * cos_t + first_half * sin_t], axis=-1)


def rms_norm(values, gain_vec):
    vals32 = values.astype(jnp.float32)
    inv_rms = lax.rsqrt(jnp.mean(vals32 * vals32, axis=-1, keepdims=True) + NORM_EPS)
    return (vals32 * inv_rms * gain_vec.astype(jnp.float32)).astype(jnp.bfloat16)


def gated_mlp(normed, w_gate, w_up, w_down):
    gate_val = jnp.dot(normed, w_gate, preferred_element_type=jnp.float32).astype(jnp.bfloat16)
    up_val = jnp.dot(normed, w_up, preferred_element_type=jnp.float32).astype(jnp.bfloat16)
    hidden_act = (jax.nn.silu(gate_val.astype(jnp.float32)) * up_val.astype(jnp.float32)).astype(jnp.bfloat16)
    return jnp.dot(hidden_act, w_down, preferred_element_type=jnp.float32)


def attend_row(queries, key_rows, val_rows, valid_mask):
    scores = jnp.einsum('kgd,tkd->kgt', queries.astype(jnp.float32), key_rows.astype(jnp.float32)) * (HEAD_DIM ** -0.5)
    scores = jnp.where(valid_mask[None, None, :], scores, NEG_BIG)
    weights = jax.nn.softmax(scores, axis=-1)
    return jnp.einsum('kgt,tkd->kgd', weights, val_rows.astype(jnp.float32))


def attend_item(item):
    return attend_row(item[0], item[1], item[2], item[3])


def dense_weight(rand_key, rows, cols):
    return (jax.random.normal(rand_key, (rows, cols), jnp.float32) * (rows ** -0.5)).astype(jnp.bfloat16)


def norm_gain(rand_key, width, center):
    return (center + 0.35 * jax.random.normal(rand_key, (width,), jnp.float32)).astype(jnp.bfloat16)


def drifting_values(rand_key, length):
    noise_key, walk_key, dir_key = jax.random.split(rand_key, 3)
    noise_part = 0.6 * jax.random.normal(noise_key, (BATCH, length, KV_HEADS, HEAD_DIM), jnp.float32)
    walk_path = jnp.cumsum(jax.random.normal(walk_key, (BATCH, KV_HEADS, length), jnp.float32), axis=-1) * (length ** -0.5)
    direction = jax.random.normal(dir_key, (BATCH, KV_HEADS, HEAD_DIM), jnp.float32)
    return (noise_part + jnp.transpose(walk_path, (0, 2, 1))[:, :, :, None] * direction[:, None, :, :]).astype(jnp.bfloat16)


def setup_inputs(seed: int = 0, part: int = 0) -> dict:
    data_keys = jax.random.split(jax.random.fold_in(jax.random.key(seed), part), 12)
    weight_keys = jax.random.split(jax.random.key(seed + 1), 20)
    row_ids = jnp.arange(BATCH)
    new_pos = jax.random.randint(data_keys[0], (BATCH,), SEQ_LEN // 4, SEQ_LEN)
    new_pos = jnp.where(row_ids == 0, SEQ_LEN - 1, new_pos).astype(jnp.int32)
    rowmask = (jax.random.randint(data_keys[1], (BATCH,), 0, 4) > 0).astype(jnp.int32)
    rowmask = jnp.where(row_ids == 0, 1, jnp.where(row_ids == 1, 0, rowmask)).astype(jnp.int32)
    valid_len = jax.random.randint(data_keys[2], (BATCH,), VIS_TOKENS // 4, VIS_TOKENS + 1)
    valid_len = jnp.where(row_ids == 0, VIS_TOKENS, valid_len)
    xvalid = (jnp.arange(VIS_TOKENS)[None, :] < valid_len[:, None]).astype(jnp.int32)
    hidden = jax.random.normal(data_keys[3], (BATCH, HIDDEN), jnp.float32).astype(jnp.bfloat16)
    k_self = (KEY_SCALE * jax.random.normal(data_keys[4], (BATCH, SEQ_LEN, KV_HEADS, HEAD_DIM), jnp.float32)).astype(jnp.bfloat16)
    v_self = drifting_values(data_keys[5], SEQ_LEN)
    k_cross = (KEY_SCALE * jax.random.normal(data_keys[6], (BATCH, VIS_TOKENS, KV_HEADS, HEAD_DIM), jnp.float32)).astype(jnp.bfloat16)
    v_cross = drifting_values(data_keys[7], VIS_TOKENS)
    return dict(
        hidden=hidden,
        new_pos=new_pos,
        k_self=k_self,
        v_self=v_self,
        k_cross=k_cross,
        v_cross=v_cross,
        xvalid=xvalid,
        rowmask=rowmask,
        self_attn_norm=norm_gain(weight_keys[0], HIDDEN, 1.0),
        self_wq=dense_weight(weight_keys[1], HIDDEN, Q_WIDTH),
        self_wk=dense_weight(weight_keys[2], HIDDEN, KV_WIDTH),
        self_wv=dense_weight(weight_keys[3], HIDDEN, KV_WIDTH),
        self_wo=dense_weight(weight_keys[4], Q_WIDTH, HIDDEN),
        self_mlp_norm=norm_gain(weight_keys[5], HIDDEN, 1.0),
        self_wgate=dense_weight(weight_keys[6], HIDDEN, MLP_DIM),
        self_wup=dense_weight(weight_keys[7], HIDDEN, MLP_DIM),
        self_wdown=dense_weight(weight_keys[8], MLP_DIM, HIDDEN),
        cross_attn_norm=norm_gain(weight_keys[9], HIDDEN, 1.0),
        cross_wq=dense_weight(weight_keys[10], HIDDEN, Q_WIDTH),
        cross_qnorm=norm_gain(weight_keys[11], HEAD_DIM, 1.5),
        cross_wo=dense_weight(weight_keys[12], Q_WIDTH, HIDDEN),
        cross_gates=jax.random.uniform(weight_keys[13], (2,), jnp.float32, 0.5, 1.5),
        cross_mlp_norm=norm_gain(weight_keys[14], HIDDEN, 1.0),
        cross_wgate=dense_weight(weight_keys[15], HIDDEN, MLP_DIM),
        cross_wup=dense_weight(weight_keys[16], HIDDEN, MLP_DIM),
        cross_wdown=dense_weight(weight_keys[17], MLP_DIM, HIDDEN),
    )


def reference(hidden, new_pos, k_self, v_self, k_cross, v_cross, xvalid, rowmask,
              self_attn_norm, self_wq, self_wk, self_wv, self_wo, self_mlp_norm,
              self_wgate, self_wup, self_wdown, cross_attn_norm, cross_wq, cross_qnorm,
              cross_wo, cross_gates, cross_mlp_norm, cross_wgate, cross_wup, cross_wdown):
    normed = rms_norm(hidden, self_attn_norm)
    queries = jnp.dot(normed, self_wq, preferred_element_type=jnp.float32).astype(jnp.bfloat16)
    key_new = jnp.dot(normed, self_wk, preferred_element_type=jnp.float32).astype(jnp.bfloat16)
    val_new = jnp.dot(normed, self_wv, preferred_element_type=jnp.float32).astype(jnp.bfloat16)
    queries = apply_rope(queries.reshape(BATCH, HEADS, HEAD_DIM).astype(jnp.float32), new_pos).astype(jnp.bfloat16)
    key_new = apply_rope(key_new.reshape(BATCH, KV_HEADS, HEAD_DIM).astype(jnp.float32), new_pos).astype(jnp.bfloat16)
    val_new = val_new.reshape(BATCH, KV_HEADS, HEAD_DIM)
    slot_ids = jnp.arange(SEQ_LEN)
    hit_mask = (slot_ids[None, :] == new_pos[:, None])[:, :, None, None]
    k_new_cache = jnp.where(hit_mask, key_new[:, None], k_self)
    v_new_cache = jnp.where(hit_mask, val_new[:, None], v_self)
    seen_mask = slot_ids[None, :] <= new_pos[:, None]
    self_out = lax.map(attend_item, (queries.reshape(BATCH, KV_HEADS, GROUP_SIZE, HEAD_DIM), k_new_cache, v_new_cache, seen_mask))
    self_flat = self_out.astype(jnp.bfloat16).reshape(BATCH, Q_WIDTH)
    after_attn = (hidden.astype(jnp.float32) + jnp.dot(self_flat, self_wo, preferred_element_type=jnp.float32)).astype(jnp.bfloat16)
    mlp_out = gated_mlp(rms_norm(after_attn, self_mlp_norm), self_wgate, self_wup, self_wdown)
    after_mlp = (after_attn.astype(jnp.float32) + mlp_out).astype(jnp.bfloat16)
    normed = rms_norm(after_mlp, cross_attn_norm)
    cross_q = jnp.dot(normed, cross_wq, preferred_element_type=jnp.float32).astype(jnp.bfloat16)
    cross_q = rms_norm(cross_q.reshape(BATCH, HEADS, HEAD_DIM), cross_qnorm)
    cross_out = lax.map(attend_item, (cross_q.reshape(BATCH, KV_HEADS, GROUP_SIZE, HEAD_DIM), k_cross, v_cross, xvalid > 0))
    cross_flat = cross_out.astype(jnp.bfloat16).reshape(BATCH, Q_WIDTH)
    gate_vals = jnp.tanh(cross_gates.astype(jnp.float32))
    row_scale = rowmask.astype(jnp.float32)[:, None]
    cross_proj = jnp.dot(cross_flat, cross_wo, preferred_element_type=jnp.float32)
    after_cross = (after_mlp.astype(jnp.float32) + gate_vals[0] * row_scale * cross_proj).astype(jnp.bfloat16)
    xmlp_out = gated_mlp(rms_norm(after_cross, cross_mlp_norm), cross_wgate, cross_wup, cross_wdown)
    after_xmlp = (after_cross.astype(jnp.float32) + gate_vals[1] * row_scale * xmlp_out).astype(jnp.bfloat16)
    return (after_xmlp, k_new_cache, v_new_cache)
```

```python
import functools
import math
import jax
import jax.numpy as jnp
from jax import lax
from jax.experimental import pallas as pl
from jax.experimental.pallas import tpu as pltpu
from jax.sharding import PartitionSpec as P

NORM_EPS = 1e-5
ROPE_THETA = 500000.0
ROPE_FACTOR = 8.0
LOW_FREQ = 1.0
HIGH_FREQ = 4.0
ORIG_CTX = 8192.0
NEG_BIG = -1e30
MESH = pl.DeviceIdType.MESH
BF = jnp.bfloat16
F32 = jnp.float32
LANES = 128
GROUP_ROWS = 8
TILE_N = 256
PAIR_SLOTS = 5
NT_DIMS = (((1,), (1,)), ((), ()))
ORDER = ((2, 0), (2, 1), (1, 0), (1, 1), (3, 0), (3, 1), (0, 1), (0, 0))


def rope_freqs(head_dim):
    inv_freq = 1.0 / (ROPE_THETA ** (jnp.arange(0, head_dim, 2).astype(jnp.float32) / head_dim))
    wavelen = 2.0 * math.pi / inv_freq
    smooth = (ORIG_CTX / wavelen - LOW_FREQ) / (HIGH_FREQ - LOW_FREQ)
    mid_freq = (1.0 - smooth) * inv_freq / ROPE_FACTOR + smooth * inv_freq
    scaled = jnp.where(wavelen > ORIG_CTX / LOW_FREQ, inv_freq / ROPE_FACTOR, mid_freq)
    return jnp.where(wavelen < ORIG_CTX / HIGH_FREQ, inv_freq, scaled)


def self_kernel(pos_sm, hid_ref, g_ref, cos_ref, sin_ref, lpv_ref, wq_hbm, wk_hbm, wv_hbm, ks_hbm, vs_hbm,
                part_ref, ko_hbm, vo_hbm,
                xb, wq_b, wk_b, wv_b, kb, vb, q_s, kn_s, vn_s, w_sem, c_sem, o_sem, *, chunks, heads, scale):
    rows, hidden = hid_ref.shape
    hd = LANES
    tlen = kb.shape[0] // rows
    kc = hidden // chunks
    loads = []
    for i in range(chunks):
        sl = pl.ds(i * kc, kc)
        loads.append([pltpu.make_async_copy(wq_hbm.at[sl], wq_b.at[sl], w_sem.at[i, 0]),
                      pltpu.make_async_copy(wk_hbm.at[sl], wk_b.at[sl], w_sem.at[i, 1]),
                      pltpu.make_async_copy(wv_hbm.at[sl], wv_b.at[sl], w_sem.at[i, 2])])
        for cp in loads[-1]:
            cp.start()
    k_in = pltpu.make_async_copy(ks_hbm, kb, c_sem.at[0])
    v_in = pltpu.make_async_copy(vs_hbm, vb, c_sem.at[1])
    k_in.start()
    v_in.start()
    h32 = hid_ref[...].astype(F32)
    inv = lax.rsqrt(jnp.mean(h32 * h32, axis=-1, keepdims=True) + NORM_EPS)
    xb[...] = (h32 * inv * g_ref[...].astype(F32)).astype(BF)
    qa = ka = va = None
    for i in range(chunks):
        for cp in loads[i]:
            cp.wait()
        sl = pl.ds(i * kc, kc)
        xi = xb[:, i * kc:(i + 1) * kc]
        q_i = jnp.dot(xi, wq_b[sl], preferred_element_type=F32)
        k_i = jnp.dot(xi, wk_b[sl], preferred_element_type=F32)
        v_i = jnp.dot(xi, wv_b[sl], preferred_element_type=F32)
        qa, ka, va = (q_i, k_i, v_i) if i == 0 else (qa + q_i, ka + k_i, va + v_i)
    cos_t = cos_ref[...]
    sin_t = sin_ref[...]

    def rope(v):
        v = v.astype(BF).astype(F32)
        return (v * cos_t + pltpu.roll(v, hd // 2, 1) * sin_t).astype(BF).astype(F32)

    for h in range(heads):
        q_s[h] = rope(qa[:, h * hd:(h + 1) * hd])
    kn_s[...] = rope(ka)
    vn_s[...] = va.astype(BF).astype(F32)
    k_in.wait()
    v_in.wait()
    gr = GROUP_ROWS
    span = gr * tlen
    t_iota = lax.broadcasted_iota(jnp.int32, (tlen, hd), 0)
    col = lax.broadcasted_iota(jnp.int32, (heads * gr, span), 1)
    row = lax.broadcasted_iota(jnp.int32, (heads * gr, span), 0)
    same = (col // tlen) == (row % gr)
    tcol = col % tlen
    lane = lax.broadcasted_iota(jnp.int32, (gr, LANES), 1)

    def group(g, carry):
        base = pl.multiple_of(g * gr, gr)
        for i in range(gr):
            hit = t_iota == pos_sm[base + i]
            sl = pl.ds(pl.multiple_of((base + i) * tlen, tlen), tlen)
            kb[sl, :] = jnp.where(hit, kn_s[pl.ds(base + i, 1), :], kb[sl, :].astype(F32)).astype(BF)
            vb[sl, :] = jnp.where(hit, vn_s[pl.ds(base + i, 1), :], vb[sl, :].astype(F32)).astype(BF)
        gs = pl.ds(pl.multiple_of(g * span, span), span)
        rs = pl.ds(base, gr)
        qg = jnp.concatenate([q_s[h, rs, :] for h in range(heads)], axis=0).astype(BF)
        s = lax.dot_general(qg, kb[gs, :], NT_DIMS, preferred_element_type=F32) * scale
        lp = lpv_ref[rs, :]
        lp = jnp.concatenate([lp] * heads, axis=0)
        lp = jnp.concatenate([lp] * (span // LANES), axis=1)
        ok = jnp.logical_and(same, tcol <= lp)
        s = jnp.where(ok, s, NEG_BIG)
        m = jnp.max(s, axis=-1, keepdims=True)
        p = jnp.where(ok, jnp.exp(s - m), 0.0)
        l = jnp.sum(p, axis=-1, keepdims=True)
        o = jnp.dot(p.astype(BF), vb[gs, :], preferred_element_type=F32)
        stat = jnp.zeros((gr, LANES), F32)
        for h in range(heads):
            hs = slice(h * gr, (h + 1) * gr)
            part_ref[rs, h * hd:(h + 1) * hd] = o[hs]
            stat = jnp.where(lane == h, m[hs], stat)
            stat = jnp.where(lane == heads + h, l[hs], stat)
        part_ref[rs, heads * hd:] = stat
        return carry

    lax.fori_loop(0, rows // gr, group, 0)
    k_out = pltpu.make_async_copy(kb, ko_hbm, o_sem.at[0])
    v_out = pltpu.make_async_copy(vb, vo_hbm, o_sem.at[1])
    k_out.start()
    v_out.start()
    k_out.wait()
    v_out.wait()


def self_phase(pos, hid, gain, cos2, sin2, lpv, wq, wk, wv, ks, vs, *, scale):
    rows, hidden = hid.shape
    tlen = ks.shape[1]
    hd = ks.shape[2]
    heads = wq.shape[1] // hd
    chunks = 4
    ks = ks.reshape(rows * tlen, hd)
    vs = vs.reshape(rows * tlen, hd)
    vm = pl.BlockSpec(memory_space=pltpu.VMEM)
    anys = pl.BlockSpec(memory_space=pl.ANY)
    cache = jax.ShapeDtypeStruct(ks.shape, BF)
    part, ko, vo = pl.pallas_call(
        functools.partial(self_kernel, chunks=chunks, heads=heads, scale=scale),
        out_shape=(jax.ShapeDtypeStruct((rows, heads * hd + LANES), F32), cache, cache),
        in_specs=[pl.BlockSpec(memory_space=pltpu.SMEM)] + [vm] * 5 + [anys] * 5,
        out_specs=(vm, anys, anys),
        scratch_shapes=[
            pltpu.VMEM((rows, hidden), BF),
            pltpu.VMEM(wq.shape, BF), pltpu.VMEM(wk.shape, BF), pltpu.VMEM(wv.shape, BF),
            pltpu.VMEM(ks.shape, BF), pltpu.VMEM(vs.shape, BF),
            pltpu.VMEM((heads, rows, hd), F32), pltpu.VMEM((rows, hd), F32), pltpu.VMEM((rows, hd), F32),
            pltpu.SemaphoreType.DMA((chunks, 3)), pltpu.SemaphoreType.DMA((2,)), pltpu.SemaphoreType.DMA((2,)),
        ],
        compiler_params=pltpu.CompilerParams(vmem_limit_bytes=30 << 20),
        name="self_attention",
    )(pos, hid, gain, cos2, sin2, lpv, wq, wk, wv, ks, vs)
    return part, ko, vo


def step_kernel(part_ref, g2_ref, g3_ref, g4_ref, qn_ref, sc0_ref, sc1_ref, xv_ref,
                hid_hbm, wo_hbm, wg_hbm, wu_hbm, wd_hbm, wqc_hbm, woc_hbm, wgc_hbm, wuc_hbm, wdc_hbm, kc_hbm, vc_hbm,
                out_ref,
                wo_b, pair_b, down_b, kc_b, vc_b, hid_b, comb, sbuf, rbuf, piece, full, xb, act, ob, of, fin,
                wo_sem, pair_sem, down_sem, kv_sem, hid_sem, cs_sem, cr_sem, rs_ssem, rs_rsem, ag_ssem, ag_rsem,
                fd_ssem, fd_rsem, ff_ssem, ff_rsem, fc_ssem, fc_rsem, *, n_sp, n_tp, heads, scale):
    sp = lax.axis_index("sp")
    tp = lax.axis_index("tp")
    xx = tp // 2
    cc = tp % 2
    n_x = n_tp // 2
    rows = hid_b.shape[0]
    wide = hid_b.shape[1]
    hd = LANES
    gr = GROUP_ROWS
    r0 = pl.multiple_of(sp * rows, rows)
    n_pairs = wg_hbm.shape[1] // TILE_N

    def tp_at(k):
        dx, dc = ORDER[k]
        return ((xx + dx) % n_x) * 2 + (cc + dc) % 2

    def remote(src, dst, ssem, rsem, **dev):
        return pltpu.make_async_remote_copy(src_ref=src, dst_ref=dst, send_sem=ssem, recv_sem=rsem,
                                            device_id=dev, device_id_type=MESH)

    def pair_copies(p):
        slot = p % PAIR_SLOTS
        if p < n_pairs:
            a, b, c0 = wg_hbm, wu_hbm, (p * TILE_N, p * TILE_N)
        elif p == n_pairs:
            a, b, c0 = wqc_hbm, wqc_hbm, (0, TILE_N)
        else:
            q = p - n_pairs - 1
            a, b, c0 = wgc_hbm, wuc_hbm, (q * TILE_N, q * TILE_N)
        return [pltpu.make_async_copy(a.at[:, pl.ds(c0[0], TILE_N)], pair_b.at[slot, 0], pair_sem.at[slot, 0]),
                pltpu.make_async_copy(b.at[:, pl.ds(c0[1], TILE_N)], pair_b.at[slot, 1], pair_sem.at[slot, 1])]

    total_pairs = 2 * n_pairs + 1

    def start_pair(p):
        if p < total_pairs:
            for cp in pair_copies(p):
                cp.start()

    def down_copy(layer, k):
        src = (wd_hbm, wdc_hbm)[layer]
        return pltpu.make_async_copy(src.at[:, pl.ds(pl.multiple_of(tp_at(k) * wide, LANES), wide)],
                                     down_b.at[k], down_sem.at[k])

    wo_copy = pltpu.make_async_copy(wo_hbm, wo_b, wo_sem)
    woc_copy = pltpu.make_async_copy(woc_hbm, wo_b, wo_sem)
    hid_copy = pltpu.make_async_copy(
        hid_hbm.at[pl.ds(r0, rows), pl.ds(pl.multiple_of(tp * wide, LANES), wide)], hid_b, hid_sem)
    kc_copy = pltpu.make_async_copy(kc_hbm.at[pl.ds(r0, rows)], kc_b, kv_sem.at[0])
    vc_copy = pltpu.make_async_copy(vc_hbm.at[pl.ds(r0, rows)], vc_b, kv_sem.at[1])
    wo_copy.start()
    hid_copy.start()
    for p in range(PAIR_SLOTS):
        start_pair(p)
    for k in range(n_tp):
        down_copy(0, k).start()
    kc_copy.start()
    vc_copy.start()

    bar = pltpu.get_barrier_semaphore()
    for j in range(1, n_sp):
        pl.semaphore_signal(bar, inc=1, device_id={"sp": (sp + j) % n_sp}, device_id_type=MESH)
    for k in range(n_tp - 1):
        pl.semaphore_signal(bar, inc=1, device_id={"tp": tp_at(k)}, device_id_type=MESH)
    pl.semaphore_wait(bar, n_sp - 1 + n_tp - 1)

    sends = []
    for j in range(1, n_sp):
        peer = (sp + j) % n_sp
        cp = remote(part_ref.at[pl.ds(pl.multiple_of(peer * rows, rows), rows)], comb.at[j - 1],
                    cs_sem.at[j - 1], cr_sem.at[j - 1], sp=peer)
        cp.start()
        sends.append(cp)
    for cp in sends:
        cp.wait()
    own = part_ref[pl.ds(r0, rows), :]
    blocks = [own] + [comb[j] for j in range(n_sp - 1)]
    qw = heads * hd
    for h in range(heads):
        ms = [b[:, qw + h:qw + h + 1] for b in blocks]
        top = functools.reduce(jnp.maximum, ms)
        fs = [jnp.exp(m - top) for m in ms]
        den = sum(b[:, qw + heads + h:qw + heads + h + 1] * f for b, f in zip(blocks, fs))
        num = sum(b[:, h * hd:(h + 1) * hd] * f for b, f in zip(blocks, fs))
        ob[:, h * hd:(h + 1) * hd] = (num / den).astype(BF)

    def reduce_scatter(product):
        sent = []
        for k in range(n_tp - 1):
            sbuf[k] = product(k)
            cp = remote(sbuf.at[k], rbuf.at[k], rs_ssem.at[k], rs_rsem.at[k], tp=tp_at(k))
            cp.start()
            sent.append(cp)
        acc = product(n_tp - 1)
        for k in reversed(range(n_tp - 1)):
            sent[k].wait()
            acc = acc + rbuf[k]
        return acc

    def share(cur, slot):
        piece[slot] = cur
        full[tp] = cur
        sent = []
        for k in range(n_tp - 1):
            cp = remote(piece.at[slot], full.at[tp], ag_ssem.at[k], ag_rsem.at[k], tp=tp_at(k))
            cp.start()
            sent.append(cp)
        for cp in sent:
            cp.wait()

    def normed(g_ref):
        acc = jnp.zeros((rows, LANES), F32)
        for j in range(n_tp):
            v = full[j]
            v = v * v
            for i in range(wide // LANES):
                acc = acc + v[:, i * LANES:(i + 1) * LANES]
        inv = lax.rsqrt(jnp.sum(acc, axis=-1, keepdims=True) * (1.0 / (n_tp * wide)) + NORM_EPS)
        for j in range(n_tp):
            sl = slice(j * wide, (j + 1) * wide)
            xb[:, sl] = (full[j] * inv * g_ref[:, sl].astype(F32)).astype(BF)

    def gate_up(first):
        for t in range(n_pairs):
            p = first + t
            slot = p % PAIR_SLOTS
            for cp in pair_copies(p):
                cp.wait()
            gate = jnp.dot(xb[...], pair_b[slot, 0], preferred_element_type=F32).astype(BF).astype(F32)
            up = jnp.dot(xb[...], pair_b[slot, 1], preferred_element_type=F32).astype(BF).astype(F32)
            act[:, t * TILE_N:(t + 1) * TILE_N] = (gate * jax.nn.sigmoid(gate) * up).astype(BF)
            start_pair(p + PAIR_SLOTS)

    def down(layer):
        def product(k):
            down_copy(layer, k).wait()
            out = jnp.dot(act[...], down_b[k], preferred_element_type=F32)
            if layer == 0:
                down_copy(1, k).start()
            return out
        return reduce_scatter(product)

    def wo_product(k):
        return jnp.dot(ob[...], wo_b[:, pl.ds(pl.multiple_of(tp_at(k) * wide, LANES), wide)],
                       preferred_element_type=F32)

    def rounded(v):
        return v.astype(BF).astype(F32)

    wo_copy.wait()
    acc = reduce_scatter(wo_product)
    woc_copy.start()
    hid_copy.wait()
    share(rounded(hid_b[...].astype(F32) + acc), 0)
    normed(g2_ref)
    gate_up(0)
    acc = down(0)
    share(rounded(piece[0] + acc), 1)

    normed(g3_ref)
    p = n_pairs
    for cp in pair_copies(p):
        cp.wait()
    for i in range(2):
        qq = jnp.dot(xb[...], pair_b[p % PAIR_SLOTS, i], preferred_element_type=F32)
        for h in range(TILE_N // hd):
            v = rounded(qq[:, h * hd:(h + 1) * hd])
            inv = lax.rsqrt(jnp.mean(v * v, axis=-1, keepdims=True) + NORM_EPS)
            of[i * (TILE_N // hd) + h] = rounded(v * inv * qn_ref[...].astype(F32))
    start_pair(p + PAIR_SLOTS)
    kc_copy.wait()
    vc_copy.wait()
    n_vis = kc_b.shape[1]
    rmod = lax.broadcasted_iota(jnp.int32, (heads * gr, n_vis), 0) % gr
    for g in range(rows // gr):
        qg = jnp.concatenate([of[h, g * gr:(g + 1) * gr] for h in range(heads)], axis=0).astype(BF)
        s = jnp.zeros((heads * gr, n_vis), F32)
        for i in range(gr):
            s_i = lax.dot_general(qg, kc_b[g * gr + i], NT_DIMS, preferred_element_type=F32)
            s = jnp.where(rmod == i, s_i, s)
        valid = xv_ref[pl.ds(pl.multiple_of(r0 + g * gr, gr), gr), :]
        ok = jnp.concatenate([valid] * heads, axis=0) > 0
        s = jnp.where(ok, s * scale, NEG_BIG)
        m = jnp.max(s, axis=-1, keepdims=True)
        pr = jnp.where(ok, jnp.exp(s - m), 0.0)
        l = jnp.sum(pr, axis=-1, keepdims=True)
        o = jnp.zeros((heads * gr, hd), F32)
        for i in range(gr):
            o = o + jnp.dot(jnp.where(rmod == i, pr, 0.0).astype(BF), vc_b[g * gr + i], preferred_element_type=F32)
        o = o / l
        for h in range(heads):
            of[h, g * gr:(g + 1) * gr] = o[h * gr:(h + 1) * gr]
    for h in range(heads):
        ob[:, h * hd:(h + 1) * hd] = of[h].astype(BF)
    woc_copy.wait()
    acc = reduce_scatter(wo_product)
    s0 = sc0_ref[pl.ds(r0, rows), 0:1]
    share(rounded(piece[1] + s0 * acc), 0)

    normed(g4_ref)
    gate_up(n_pairs + 1)
    acc = down(1)
    s1 = sc1_ref[pl.ds(r0, rows), 0:1]
    fin[cc, sp, xx] = rounded(piece[0] + s1 * acc)

    half = rows // 2
    top = pl.ds(0, half)
    bot = pl.ds(half, half)

    def hop_x(src_sp, src_x, part, dx, ssem, rsem):
        blk = fin.at[cc, src_sp, src_x, part]
        return remote(blk, blk, ssem, rsem, tp=((xx + dx) % n_x) * 2 + cc)

    def hop_y(src_sp, src_x, part, dy, ssem, rsem):
        blk = fin.at[cc, src_sp, src_x, part]
        return remote(blk, blk, ssem, rsem, sp=(sp + dy) % n_sp)

    steps = (2, 1, 3)
    first = []
    for i, d in enumerate(steps):
        cx = hop_x(sp, xx, top, d, fd_ssem.at[0, i], fd_rsem.at[0, i])
        cy = hop_y(sp, xx, bot, d, fd_ssem.at[1, i], fd_rsem.at[1, i])
        cx.start()
        cy.start()
        first.append((cx, cy))
    second = []

    def forward(a, from_x, from_y):
        for i, d in enumerate(steps):
            cy = hop_y(sp, from_x, top, d, ff_ssem.at[0, a, i], ff_rsem.at[0, a, i])
            cx = hop_x(from_y, xx, bot, d, ff_ssem.at[1, a, i], ff_rsem.at[1, a, i])
            cy.start()
            cx.start()
            second.append((cx, cy))

    forward(0, xx, sp)
    for a, i in ((1, 1), (2, 2), (3, 0)):
        cx, cy = first[i]
        cx.wait()
        cy.wait()
        forward(a, (xx + n_x - steps[i]) % n_x, (sp + n_sp - steps[i]) % n_sp)
    for cx, cy in second:
        cx.wait()
        cy.wait()
    cp = remote(fin.at[cc], fin.at[cc], fc_ssem, fc_rsem, tp=xx * 2 + (1 - cc))
    cp.start()
    cp.wait()
    for c in range(2):
        for s in range(n_sp):
            for x in range(n_x):
                j = x * 2 + c
                out_ref[s * rows:(s + 1) * rows, j * wide:(j + 1) * wide] = fin[c, s, x].astype(BF)


def step_phase(part, gains, qnorm, sc0, sc1, xvalid, hid, weights, kc, vc, *, n_sp, n_tp, heads, scale):
    all_rows, hidden = hid.shape
    rows = all_rows // n_sp
    wide = hidden // n_tp
    mlp = weights[1].shape[1]
    n_vis, hd = kc.shape[1], kc.shape[2]
    vm = pl.BlockSpec(memory_space=pltpu.VMEM)
    anys = pl.BlockSpec(memory_space=pl.ANY)
    dma = pltpu.SemaphoreType.DMA
    n_x = n_tp // 2
    peers = n_tp - 1
    return pl.pallas_call(
        functools.partial(step_kernel, n_sp=n_sp, n_tp=n_tp, heads=heads, scale=scale),
        out_shape=jax.ShapeDtypeStruct((all_rows, hidden), BF),
        in_specs=[vm] * 8 + [anys] * 12,
        out_specs=vm,
        scratch_shapes=[
            pltpu.VMEM(weights[0].shape, BF),
            pltpu.VMEM((PAIR_SLOTS, 2, hidden, TILE_N), BF),
            pltpu.VMEM((n_tp, mlp, wide), BF),
            pltpu.VMEM((rows, n_vis, hd), BF), pltpu.VMEM((rows, n_vis, hd), BF),
            pltpu.VMEM((rows, wide), BF),
            pltpu.VMEM((n_sp - 1, rows, part.shape[1]), F32),
            pltpu.VMEM((peers, rows, wide), F32), pltpu.VMEM((peers, rows, wide), F32),
            pltpu.VMEM((2, rows, wide), F32),
            pltpu.VMEM((n_tp, rows, wide), F32),
            pltpu.VMEM((rows, hidden), BF),
            pltpu.VMEM((rows, mlp), BF),
            pltpu.VMEM((rows, heads * hd), BF),
            pltpu.VMEM((heads, rows, hd), F32),
            pltpu.VMEM((2, n_sp, n_x, rows, wide), F32),
            dma, dma((PAIR_SLOTS, 2)), dma((n_tp,)), dma((2,)), dma,
            dma((n_sp - 1,)), dma((n_sp - 1,)), dma((peers,)), dma((peers,)), dma((peers,)), dma((peers,)),
            dma((2, 3)), dma((2, 3)), dma((2, 4, 3)), dma((2, 4, 3)), dma, dma,
        ],
        compiler_params=pltpu.CompilerParams(collective_id=1, has_side_effects=True, vmem_limit_bytes=67043328),
        name="decode_step",
    )(part, *gains, qnorm, sc0, sc1, xvalid, hid, *weights, kc, vc)


def solution(mesh):
    cache_spec = P('dp', 'sp', 'tp', None)
    cross_spec = P('dp', None, 'tp', None)
    row_spec = P('dp', None)
    vec_spec = P('dp')
    full_spec = P(None)
    col_spec = P(None, 'tp')
    split_rows = P('tp', None)
    in_specs = (row_spec, vec_spec, cache_spec, cache_spec, cross_spec, cross_spec, row_spec, vec_spec,
                full_spec, col_spec, col_spec, col_spec, split_rows, full_spec, col_spec, col_spec, split_rows,
                full_spec, col_spec, full_spec, split_rows, full_spec, full_spec, col_spec, col_spec, split_rows)
    out_specs = (row_spec, cache_spec, cache_spec)
    n_sp = mesh.shape['sp']
    n_tp = mesh.shape['tp']

    def local_step(hidden, new_pos, k_self, v_self, k_cross, v_cross, xvalid, rowmask,
                   self_attn_norm, self_wq, self_wk, self_wv, self_wo, self_mlp_norm,
                   self_wgate, self_wup, self_wdown, cross_attn_norm, cross_wq, cross_qnorm,
                   cross_wo, cross_gates, cross_mlp_norm, cross_wgate, cross_wup, cross_wdown):
        batch_rows = hidden.shape[0]
        len_local = k_self.shape[1]
        head_dim = k_self.shape[3]
        heads = self_wq.shape[1] // head_dim
        scale = head_dim ** -0.5
        angles = new_pos.astype(F32)[:, None] * rope_freqs(head_dim)[None, :]
        cos_t = jnp.cos(angles)
        sin_t = jnp.sin(angles)
        cos2 = jnp.concatenate([cos_t, cos_t], axis=-1)
        sin2 = jnp.concatenate([-sin_t, sin_t], axis=-1)
        local_pos = new_pos - lax.axis_index('sp') * len_local
        lpv = jnp.broadcast_to(local_pos[:, None], (batch_rows, LANES))
        flat = (batch_rows, len_local, head_dim)
        part, ko, vo = self_phase(local_pos, hidden, self_attn_norm[None, :], cos2, sin2, lpv, self_wq, self_wk, self_wv,
                                  k_self.reshape(flat), v_self.reshape(flat), scale=scale)
        gate_vals = jnp.tanh(cross_gates.astype(F32))
        row_scale = jnp.broadcast_to(rowmask.astype(F32)[:, None], (batch_rows, LANES))
        gains = (self_mlp_norm[None, :], cross_attn_norm[None, :], cross_mlp_norm[None, :])
        weights = (self_wo, self_wgate, self_wup, self_wdown, cross_wq, cross_wo, cross_wgate, cross_wup, cross_wdown)
        cflat = (batch_rows, k_cross.shape[1], head_dim)
        h4 = step_phase(part, gains, cross_qnorm[None, :], gate_vals[0] * row_scale, gate_vals[1] * row_scale, xvalid,
                        hidden, weights, k_cross.reshape(cflat), v_cross.reshape(cflat),
                        n_sp=n_sp, n_tp=n_tp, heads=heads, scale=scale)
        return h4, ko.reshape(k_self.shape), vo.reshape(v_self.shape)

    return jax.shard_map(local_step, mesh=mesh, in_specs=in_specs, out_specs=out_specs, check_vma=False)
```

```python
import functools
import math
import jax
import jax.numpy as jnp
import numpy as np
from jax import lax
from jax.experimental import pallas as pl
from jax.experimental.pallas import tpu as pltpu
from jax.sharding import PartitionSpec as P

NORM_EPS = 1e-5
ROPE_THETA = 500000.0
ROPE_FACTOR = 8.0
LOW_FREQ = 1.0
HIGH_FREQ = 4.0
ORIG_CTX = 8192.0
NEG_BIG = -1e30
MESH = pl.DeviceIdType.MESH
BF = jnp.bfloat16
F32 = jnp.float32
LANES = 128
GROUP_ROWS = 8
CHUNK_SLOTS = 5
NT_DIMS = (((1,), (1,)), ((), ()))
ORDER = ((0, 0), (0, 1), (1, 0), (3, 0), (1, 1), (3, 1), (2, 0), (2, 1))
FROM = (0, 1, 3, 2, 5, 4, 6, 7)
CHIPS = (2, 1, 3, 0)


def rope_table(head_dim):
    inv_freq = (1.0 / (ROPE_THETA ** (np.arange(0, head_dim, 2) / head_dim))).astype(np.float32)
    wavelen = 2.0 * math.pi / inv_freq
    smooth = (ORIG_CTX / wavelen - LOW_FREQ) / (HIGH_FREQ - LOW_FREQ)
    mid_freq = (1.0 - smooth) * inv_freq / ROPE_FACTOR + smooth * inv_freq
    scaled = np.where(wavelen > ORIG_CTX / LOW_FREQ, inv_freq / ROPE_FACTOR, mid_freq)
    freqs = np.where(wavelen < ORIG_CTX / HIGH_FREQ, inv_freq, scaled)
    table = np.zeros((8, head_dim), np.float32)
    table[0] = np.concatenate([freqs, freqs])
    table[1] = np.where(np.arange(head_dim) < head_dim // 2, -1.0, 1.0)
    return jnp.asarray(table)


def self_kernel(pos_sm, freq_hbm, hid_hbm, g_hbm, wq_hbm, wk_hbm, wv_hbm, ks_hbm, vs_hbm,
                part_hbm, ko_hbm, vo_hbm,
                freq_b, hid_b, g_b, xb, w_b, wk_b, wv_b, kb, vb, q_s, kn_s, vn_s, lp_s, s_s, part_b,
                i_sem, w_sem, c_sem, o_sem, *, chunks, heads, scale):
    rows, hidden = hid_b.shape
    hd = LANES
    tlen = kb.shape[0] // rows
    kc = hidden // chunks
    qw = heads * hd
    small = [pltpu.make_async_copy(hid_hbm, hid_b, i_sem.at[0]), pltpu.make_async_copy(g_hbm, g_b, i_sem.at[1]),
             pltpu.make_async_copy(freq_hbm, freq_b, i_sem.at[2])]
    for cp in small:
        cp.start()
    kv_in = [pltpu.make_async_copy(wk_hbm, wk_b, i_sem.at[3]), pltpu.make_async_copy(wv_hbm, wv_b, i_sem.at[4]),
             pltpu.make_async_copy(ks_hbm, kb, c_sem.at[0]), pltpu.make_async_copy(vs_hbm, vb, c_sem.at[1])]
    for cp in kv_in:
        cp.start()
    loads = []
    for i in range(chunks):
        sl = pl.ds(i * kc, kc)
        loads.append(pltpu.make_async_copy(wq_hbm.at[sl], w_b.at[sl], w_sem.at[i]))
        loads[-1].start()
    for cp in small:
        cp.wait()
    acc = jnp.zeros((rows, LANES), F32)
    for c in range(hidden // LANES):
        v = hid_b[:, c * LANES:(c + 1) * LANES].astype(F32)
        acc = acc + v * v
    inv = lax.rsqrt(jnp.sum(acc, axis=-1, keepdims=True) * (1.0 / hidden) + NORM_EPS)
    g_all = g_b[...].astype(F32)
    for c in range(hidden // LANES):
        sl = slice(c * LANES, (c + 1) * LANES)
        xb[:, sl] = (hid_b[:, sl].astype(F32) * inv * g_all[c:c + 1, :]).astype(BF)
    gr = GROUP_ROWS
    sub = lax.broadcasted_iota(jnp.int32, (gr, LANES), 0)
    pos_rows = []
    for g in range(rows // gr):
        pg = jnp.zeros((gr, LANES), jnp.int32)
        for i in range(gr):
            pg = jnp.where(sub == i, pos_sm[g * gr + i], pg)
        pos_rows.append(pg)
    pos_v = jnp.concatenate(pos_rows, axis=0)
    first = lax.axis_index("sp") * tlen
    lp_s[...] = pos_v - first
    ang = pos_v.astype(F32) * freq_b[0:1, :]
    cos_t = jnp.cos(ang)
    sin_t = jnp.sin(ang) * freq_b[1:2, :]

    def rope(v):
        v = v.astype(BF).astype(F32)
        return (v * cos_t + pltpu.roll(v, hd // 2, 1) * sin_t).astype(BF).astype(F32)

    for cp in kv_in:
        cp.wait()
    kn_s[...] = rope(jnp.dot(xb[...], wk_b[...], preferred_element_type=F32))
    vn_s[...] = jnp.dot(xb[...], wv_b[...], preferred_element_type=F32).astype(BF).astype(F32)
    span = gr * tlen
    t_iota = lax.broadcasted_iota(jnp.int32, (tlen, hd), 0)

    def update(g, carry):
        base = pl.multiple_of(g * gr, gr)
        for i in range(gr):
            hit = t_iota == pos_sm[base + i] - first
            sl = pl.ds(pl.multiple_of((base + i) * tlen, tlen), tlen)
            kb[sl, :] = jnp.where(hit, kn_s[pl.ds(base + i, 1), :], kb[sl, :].astype(F32)).astype(BF)
            vb[sl, :] = jnp.where(hit, vn_s[pl.ds(base + i, 1), :], vb[sl, :].astype(F32)).astype(BF)
        return carry

    lax.fori_loop(0, rows // gr, update, 0)
    k_out = pltpu.make_async_copy(kb, ko_hbm, o_sem.at[0])
    v_out = pltpu.make_async_copy(vb, vo_hbm, o_sem.at[1])
    k_out.start()
    v_out.start()
    qq = None
    for i in range(chunks):
        loads[i].wait()
        part = jnp.dot(xb[:, i * kc:(i + 1) * kc], w_b[i * kc:(i + 1) * kc, :], preferred_element_type=F32)
        qq = part if qq is None else qq + part
    for h in range(heads):
        q_s[h] = rope(qq[:, h * hd:(h + 1) * hd])
    groups = rows // gr
    for g in range(groups):
        rs = slice(g * gr, (g + 1) * gr)
        qg = jnp.concatenate([q_s[h, rs, :] for h in range(heads)], axis=0).astype(BF)
        s_s[g] = lax.dot_general(qg, kb[g * span:(g + 1) * span, :], NT_DIMS, preferred_element_type=F32)
    col = lax.broadcasted_iota(jnp.int32, (heads * gr, LANES), 1)
    row = lax.broadcasted_iota(jnp.int32, (heads * gr, LANES), 0)
    lane = lax.broadcasted_iota(jnp.int32, (gr, LANES), 1)
    tcol = col % tlen
    for g in range(groups):
        rs = slice(g * gr, (g + 1) * gr)
        lp = jnp.concatenate([lp_s[rs, :]] * heads, axis=0)
        seen = tcol <= lp
        oks, ss = [], []
        for c in range(span // LANES):
            ok = jnp.logical_and(seen, c * (LANES // tlen) + col // tlen == row % gr)
            oks.append(ok)
            ss.append(jnp.where(ok, s_s[g, :, c * LANES:(c + 1) * LANES] * scale, NEG_BIG))
        m = jnp.max(functools.reduce(jnp.maximum, ss), axis=-1, keepdims=True)
        ps = [jnp.where(ok, jnp.exp(s - m), 0.0) for ok, s in zip(oks, ss)]
        l = jnp.sum(functools.reduce(jnp.add, ps), axis=-1, keepdims=True)
        p = jnp.concatenate(ps, axis=1).astype(BF)
        o = jnp.dot(p, vb[g * span:(g + 1) * span, :], preferred_element_type=F32)
        stat = jnp.zeros((gr, LANES), F32)
        for h in range(heads):
            hs = slice(h * gr, (h + 1) * gr)
            part_b[rs, h * hd:(h + 1) * hd] = o[hs]
            stat = jnp.where(lane == h, m[hs], stat)
            stat = jnp.where(lane == heads + h, l[hs], stat)
        part_b[rs, qw:] = stat
    p_out = pltpu.make_async_copy(part_b, part_hbm, o_sem.at[2])
    p_out.start()
    p_out.wait()
    k_out.wait()
    v_out.wait()


def self_phase(pos, hid, gain, wq, wk, wv, ks, vs, *, scale):
    rows, hidden = hid.shape
    tlen = ks.shape[1]
    hd = ks.shape[2]
    heads = wq.shape[1] // hd
    chunks = 4
    ks = ks.reshape(rows * tlen, hd)
    vs = vs.reshape(rows * tlen, hd)
    freq = rope_table(hd)
    anys = pl.BlockSpec(memory_space=pl.ANY)
    cache = jax.ShapeDtypeStruct(ks.shape, BF)
    pshape = (rows, heads * hd + LANES)
    return pl.pallas_call(
        functools.partial(self_kernel, chunks=chunks, heads=heads, scale=scale),
        out_shape=(jax.ShapeDtypeStruct(pshape, F32), cache, cache),
        in_specs=[pl.BlockSpec(memory_space=pltpu.SMEM)] + [anys] * 8,
        out_specs=(anys, anys, anys),
        scratch_shapes=[
            pltpu.VMEM(freq.shape, F32), pltpu.VMEM((rows, hidden), BF), pltpu.VMEM(gain.shape, BF),
            pltpu.VMEM((rows, hidden), BF), pltpu.VMEM(wq.shape, BF),
            pltpu.VMEM(wk.shape, BF), pltpu.VMEM(wv.shape, BF),
            pltpu.VMEM(ks.shape, BF), pltpu.VMEM(vs.shape, BF),
            pltpu.VMEM((heads, rows, hd), F32), pltpu.VMEM((rows, hd), F32), pltpu.VMEM((rows, hd), F32),
            pltpu.VMEM((rows, LANES), jnp.int32),
            pltpu.VMEM((rows // GROUP_ROWS, heads * GROUP_ROWS, GROUP_ROWS * tlen), F32), pltpu.VMEM(pshape, F32),
            pltpu.SemaphoreType.DMA((5,)), pltpu.SemaphoreType.DMA((chunks,)), pltpu.SemaphoreType.DMA((2,)),
            pltpu.SemaphoreType.DMA((3,)),
        ],
        compiler_params=pltpu.CompilerParams(vmem_limit_bytes=60 << 20),
        name="self_attention",
    )(pos, freq, hid, gain, wq, wk, wv, ks, vs)


def step_kernel(mask_sm, gate_sm, part_hbm, g2_hbm, g3_hbm, g4_hbm, qn_hbm, xv_hbm,
                hid_hbm, wo_hbm, wg_hbm, wu_hbm, wd_hbm, wqc_hbm, woc_hbm, wgc_hbm, wuc_hbm, wdc_hbm, kc_hbm, vc_hbm,
                out_ref,
                wo_b, chunk_b, qc_b, down_b, kc_b, vc_b, hid_b, comb, sbuf, rbuf, piece, full, stat, stats, acc_s, act, ob, of,
                fin, part_ref, gain_b, gain_f, qn_ref, xv_ref, small_sem,
                wo_sem, chunk_sem, qc_sem, down_sem, kv_sem, hid_sem, cs_sem, cr_sem, rs_ssem, rs_rsem, ag_ssem, ag_rsem,
                st_ssem, st_rsem, fd_ssem, fd_rsem, ff_ssem, ff_rsem, fc_ssem, fc_rsem, *, n_sp, n_tp, heads, scale):
    sp = lax.axis_index("sp")
    tp = lax.axis_index("tp")
    xx = tp // 2
    cc = tp % 2
    n_x = n_tp // 2
    rows = hid_b.shape[0]
    wide = hid_b.shape[1]
    mlp = act.shape[1]
    hd = LANES
    gr = GROUP_ROWS
    per = wide // LANES
    r0 = pl.multiple_of(sp * rows, rows)

    def tp_at(k):
        dx, dc = ORDER[k]
        return ((xx + dx) % n_x) * 2 + (cc + dc) % 2

    def remote(src, dst, ssem, rsem, **dev):
        return pltpu.make_async_remote_copy(src_ref=src, dst_ref=dst, send_sem=ssem, recv_sem=rsem,
                                            device_id=dev, device_id_type=MESH)

    def chunk_copies(n):
        slot = n % CHUNK_SLOTS
        a, b = ((wg_hbm, wu_hbm), (wgc_hbm, wuc_hbm))[n // n_tp]
        src = pl.ds(pl.multiple_of(tp_at(n % n_tp) * wide, wide), wide)
        return [pltpu.make_async_copy(a.at[src], chunk_b.at[slot, :, pl.ds(0, mlp)], chunk_sem.at[slot, 0]),
                pltpu.make_async_copy(b.at[src], chunk_b.at[slot, :, pl.ds(mlp, mlp)], chunk_sem.at[slot, 1])]

    def start_chunks(first, last):
        for n in range(first, last):
            for cp in chunk_copies(n):
                cp.start()

    def chip_at(i):
        return (xx + CHIPS[i]) % n_x

    def down_copy(layer, i):
        src = (wd_hbm, wdc_hbm)[layer]
        return pltpu.make_async_copy(src.at[:, pl.ds(pl.multiple_of(chip_at(i) * 2 * wide, LANES), 2 * wide)],
                                     down_b.at[i], down_sem.at[i])

    wo_copy = pltpu.make_async_copy(wo_hbm, wo_b, wo_sem)
    woc_copy = pltpu.make_async_copy(woc_hbm, wo_b, wo_sem)
    qc_copy = pltpu.make_async_copy(wqc_hbm, qc_b, qc_sem)
    hid_copy = pltpu.make_async_copy(
        hid_hbm.at[pl.ds(r0, rows), pl.ds(pl.multiple_of(tp * wide, LANES), wide)], hid_b, hid_sem)
    kc_copy = pltpu.make_async_copy(kc_hbm.at[pl.ds(r0, rows)], kc_b, kv_sem.at[0])
    vc_copy = pltpu.make_async_copy(vc_hbm.at[pl.ds(r0, rows)], vc_b, kv_sem.at[1])
    small = [pltpu.make_async_copy(part_hbm, part_ref, small_sem.at[0]),
             pltpu.make_async_copy(g2_hbm, gain_b.at[0], small_sem.at[1]),
             pltpu.make_async_copy(g3_hbm, gain_b.at[1], small_sem.at[2]),
             pltpu.make_async_copy(g4_hbm, gain_b.at[2], small_sem.at[3]),
             pltpu.make_async_copy(qn_hbm, qn_ref, small_sem.at[4]),
             pltpu.make_async_copy(xv_hbm.at[pl.ds(r0, rows)], xv_ref, small_sem.at[5])]
    for cp in small:
        cp.start()

    bar = pltpu.get_barrier_semaphore()
    for j in range(1, n_sp):
        pl.semaphore_signal(bar, inc=1, device_id={"sp": (sp + j) % n_sp}, device_id_type=MESH)
    for k in range(1, n_tp):
        pl.semaphore_signal(bar, inc=1, device_id={"tp": tp_at(k)}, device_id_type=MESH)

    wo_copy.start()
    hid_copy.start()
    start_chunks(0, 3)
    for cp in small:
        cp.wait()
    for i in range(3):
        g_all = gain_b[i].astype(F32)
        for j in range(n_tp):
            gain_f[i, j] = g_all[j * per:(j + 1) * per, :]
    pl.semaphore_wait(bar, n_sp - 1 + n_tp - 1)

    sends = []
    for i, j in enumerate((2, 1, 3)):
        peer = (sp + j) % n_sp
        cp = remote(part_ref.at[pl.ds(pl.multiple_of(peer * rows, rows), rows)], comb.at[i],
                    cs_sem.at[i], cr_sem.at[i], sp=peer)
        cp.start()
        sends.append(cp)
    start_chunks(3, CHUNK_SLOTS)
    for cp in sends:
        cp.wait()
    own = part_ref[pl.ds(r0, rows), :]
    blocks = [own] + [comb[j] for j in range(n_sp - 1)]
    qw = heads * hd
    for h in range(heads):
        ms = [b[:, qw + h:qw + h + 1] for b in blocks]
        top = functools.reduce(jnp.maximum, ms)
        fs = [jnp.exp(m - top) for m in ms]
        den = sum(b[:, qw + heads + h:qw + heads + h + 1] * f for b, f in zip(blocks, fs))
        num = sum(b[:, h * hd:(h + 1) * hd] * f for b, f in zip(blocks, fs))
        ob[:, h * hd:(h + 1) * hd] = (num / den).astype(BF)

    def reduce_scatter(product, then=None):
        sent = []
        for i in range(n_x):
            out = product(i)
            sbuf[2 * i] = out[:, :wide]
            sbuf[2 * i + 1] = out[:, wide:]
            if i < n_x - 1:
                for c in range(2):
                    cp = remote(sbuf.at[2 * i + c], rbuf.at[2 * i + cc], rs_ssem.at[2 * i + c], rs_rsem.at[2 * i + cc],
                                tp=chip_at(i) * 2 + c)
                    cp.start()
                    sent.append(cp)
        last = 2 * (n_x - 1)
        cp = remote(sbuf.at[last + 1 - cc], rbuf.at[last], rs_ssem.at[last], rs_rsem.at[last], tp=xx * 2 + 1 - cc)
        cp.start()
        sent.append(cp)
        if then is not None:
            then()
        acc = sbuf[last + cc]
        for j in (6, 2, 3, 4, 5, 0, 1):
            remote(sbuf.at[j], rbuf.at[j], rs_ssem.at[j], rs_rsem.at[j], tp=xx * 2 + 1 - cc).wait_recv()
            acc = acc + rbuf[j]
        for cp in sent:
            cp.wait_send()
        return acc

    def normed_chunks(cur, slot, gain, use):
        piece[slot] = cur
        part = jnp.sum(cur * cur, axis=-1, keepdims=True)
        stat[slot] = jnp.broadcast_to(part, (rows, LANES))
        sent = []
        for k in range(1, n_tp):
            cp = remote(stat.at[slot], stats.at[k - 1], st_ssem.at[k - 1], st_rsem.at[k - 1], tp=tp_at(k))
            cp.start()
            sent.append(cp)
        for k in range(1, n_tp):
            cp = remote(piece.at[slot], full.at[k - 1], ag_ssem.at[k - 1], ag_rsem.at[k - 1], tp=tp_at(k))
            cp.start()
            sent.append(cp)
        tot = stat[slot]
        for k in range(1, n_tp):
            sent[k - 1].wait_recv()
            tot = tot + stats[k - 1]
        inv = lax.rsqrt(tot * (1.0 / (n_tp * wide)) + NORM_EPS)
        for k in range(n_tp):
            if k == 0:
                v = cur
            else:
                j = FROM[k] - 1
                remote(piece.at[slot], full.at[j], ag_ssem.at[j], ag_rsem.at[j], tp=tp_at(k)).wait_recv()
                v = full[j]
            g = gain_f[gain, tp_at(k)]
            x = [v[:, i * LANES:(i + 1) * LANES] * inv * g[i:i + 1, :] for i in range(per)]
            use(k, jnp.concatenate(x, axis=1).astype(BF))
        for cp in sent:
            cp.wait_send()

    def gate_up(layer, cur, slot, gain):
        def use(k, x):
            n = layer * n_tp + k
            for cp in chunk_copies(n):
                cp.wait()
            out = jnp.dot(x, chunk_b[n % CHUNK_SLOTS], preferred_element_type=F32)
            if k == 0:
                acc_s[...] = out
            else:
                acc_s[...] += out
            if k + CHUNK_SLOTS < n_tp:
                start_chunks(n + CHUNK_SLOTS, n + CHUNK_SLOTS + 1)

        normed_chunks(cur, slot, gain, use)
        gate = acc_s[:, :mlp].astype(BF).astype(F32)
        up = acc_s[:, mlp:].astype(BF).astype(F32)
        act[...] = (gate * jax.nn.sigmoid(gate) * up).astype(BF)

    def load_down(layer):
        for i in range(n_x):
            down_copy(layer, i).start()

    def load_cross_mlp():
        start_chunks(n_tp, n_tp + CHUNK_SLOTS)
        load_down(1)

    def down(layer):
        def product(i):
            down_copy(layer, i).wait()
            return jnp.dot(act[...], down_b[i], preferred_element_type=F32)

        return reduce_scatter(product, load_cross_mlp if layer == 0 else None)

    def wo_product(i):
        return jnp.dot(ob[...], wo_b[:, pl.ds(pl.multiple_of(chip_at(i) * 2 * wide, LANES), 2 * wide)],
                       preferred_element_type=F32)

    def rounded(v):
        return v.astype(BF).astype(F32)

    def row_scale(i):
        sub = lax.broadcasted_iota(jnp.int32, (rows, LANES), 0)
        out = jnp.zeros((rows, LANES), jnp.int32)
        for r in range(rows):
            out = jnp.where(sub == r, mask_sm[r0 + r], out)
        return (jnp.tanh(jnp.full((rows, LANES), gate_sm[i], F32)) * out.astype(F32))[:, 0:1]

    wo_copy.wait()
    acc = reduce_scatter(wo_product, lambda: load_down(0))
    hid_copy.wait()
    gate_up(0, rounded(hid_b[...].astype(F32) + acc), 0, 0)
    woc_copy.start()
    qc_copy.start()
    kc_copy.start()
    vc_copy.start()
    acc = down(0)

    qc_copy.wait()
    q_parts = []

    def use_q(k, x):
        w = qc_b[pl.ds(pl.multiple_of(tp_at(k) * wide, wide), wide), :]
        out = jnp.dot(x, w, preferred_element_type=F32)
        q_parts[:] = [out if k == 0 else q_parts[0] + out]

    normed_chunks(rounded(piece[0] + acc), 1, 1, use_q)
    for h in range(heads):
        v = rounded(q_parts[0][:, h * hd:(h + 1) * hd])
        inv = lax.rsqrt(jnp.mean(v * v, axis=-1, keepdims=True) + NORM_EPS)
        of[h] = rounded(v * inv * qn_ref[...].astype(F32))
    kc_copy.wait()
    vc_copy.wait()
    n_vis = kc_b.shape[1]
    rmod = lax.broadcasted_iota(jnp.int32, (heads * gr, n_vis), 0) % gr
    for g in range(rows // gr):
        qg = jnp.concatenate([of[h, g * gr:(g + 1) * gr] for h in range(heads)], axis=0).astype(BF)
        s = jnp.zeros((heads * gr, n_vis), F32)
        for i in range(gr):
            s_i = lax.dot_general(qg, kc_b[g * gr + i], NT_DIMS, preferred_element_type=F32)
            s = jnp.where(rmod == i, s_i, s)
        valid = xv_ref[g * gr:(g + 1) * gr, :]
        ok = jnp.concatenate([valid] * heads, axis=0) > 0
        s = jnp.where(ok, s * scale, NEG_BIG)
        m = jnp.max(s, axis=-1, keepdims=True)
        pr = jnp.where(ok, jnp.exp(s - m), 0.0)
        l = jnp.sum(pr, axis=-1, keepdims=True)
        o = jnp.zeros((heads * gr, hd), F32)
        for i in range(gr):
            o = o + jnp.dot(jnp.where(rmod == i, pr, 0.0).astype(BF), vc_b[g * gr + i], preferred_element_type=F32)
        o = o / l
        for h in range(heads):
            of[h, g * gr:(g + 1) * gr] = o[h * gr:(h + 1) * gr]
    for h in range(heads):
        ob[:, h * hd:(h + 1) * hd] = of[h].astype(BF)
    woc_copy.wait()
    acc = reduce_scatter(wo_product)

    gate_up(1, rounded(piece[1] + row_scale(0) * acc), 0, 2)
    acc = down(1)
    fin[cc, sp, xx] = rounded(piece[0] + row_scale(1) * acc)

    half = rows // 2
    top = pl.ds(0, half)
    bot = pl.ds(half, half)

    def hop_x(src_sp, src_x, part, dx, ssem, rsem):
        blk = fin.at[cc, src_sp, src_x, part]
        return remote(blk, blk, ssem, rsem, tp=((xx + dx) % n_x) * 2 + cc)

    def hop_y(src_sp, src_x, part, dy, ssem, rsem):
        blk = fin.at[cc, src_sp, src_x, part]
        return remote(blk, blk, ssem, rsem, sp=(sp + dy) % n_sp)

    across = []

    def hop_core(src_sp, src_x, *part):
        blk = fin.at[(cc, src_sp, src_x) + part]
        i = len(across)
        cp = remote(blk, blk, fc_ssem.at[i], fc_rsem.at[i], tp=xx * 2 + (1 - cc))
        cp.start()
        across.append(cp)

    steps = (2, 1, 3)
    first = []
    for i, d in enumerate(steps):
        cx = hop_x(sp, xx, top, d, fd_ssem.at[0, i], fd_rsem.at[0, i])
        cy = hop_y(sp, xx, bot, d, fd_ssem.at[1, i], fd_rsem.at[1, i])
        cx.start()
        cy.start()
        first.append((cx, cy))
    second = []

    def forward(a, from_x, from_y):
        for i, d in enumerate(steps):
            cy = hop_y(sp, from_x, top, d, ff_ssem.at[0, a, i], ff_rsem.at[0, a, i])
            cx = hop_x(from_y, xx, bot, d, ff_ssem.at[1, a, i], ff_rsem.at[1, a, i])
            cy.start()
            cx.start()
            second.append((cx, from_y, (xx + n_x - d) % n_x, cy, (sp + n_sp - d) % n_sp, from_x))

    forward(0, xx, sp)
    hop_core(sp, xx)
    for a, i in ((1, 1), (2, 2), (3, 0)):
        cx, cy = first[i]
        from_x = (xx + n_x - steps[i]) % n_x
        from_y = (sp + n_sp - steps[i]) % n_sp
        cx.wait_recv()
        cy.wait_recv()
        forward(a, from_x, from_y)
        hop_core(sp, from_x, top)
        hop_core(from_y, xx, bot)
    for cx, b_sp, b_x, cy, t_sp, t_x in second:
        cx.wait_recv()
        hop_core(b_sp, b_x, bot)
        cy.wait_recv()
        hop_core(t_sp, t_x, top)
    for cx, cy in first:
        cx.wait_send()
        cy.wait_send()
    for cx, _, _, cy, _, _ in second:
        cx.wait_send()
        cy.wait_send()
    for cp in across:
        cp.wait()
    for c in range(2):
        for s in range(n_sp):
            for x in range(n_x):
                j = x * 2 + c
                out_ref[s * rows:(s + 1) * rows, j * wide:(j + 1) * wide] = fin[c, s, x].astype(BF)


def step_phase(mask, gates, part, gains, qnorm, xvalid, hid, weights, kc, vc, *, n_sp, n_tp, heads, scale):
    all_rows, hidden = hid.shape
    rows = all_rows // n_sp
    wide = hidden // n_tp
    mlp = weights[1].shape[1]
    n_vis, hd = kc.shape[1], kc.shape[2]
    vm = pl.BlockSpec(memory_space=pltpu.VMEM)
    anys = pl.BlockSpec(memory_space=pl.ANY)
    dma = pltpu.SemaphoreType.DMA
    n_x = n_tp // 2
    peers = n_tp - 1
    return pl.pallas_call(
        functools.partial(step_kernel, n_sp=n_sp, n_tp=n_tp, heads=heads, scale=scale),
        out_shape=jax.ShapeDtypeStruct((all_rows, hidden), BF),
        in_specs=[pl.BlockSpec(memory_space=pltpu.SMEM)] * 2 + [anys] * 18,
        out_specs=vm,
        scratch_shapes=[
            pltpu.VMEM(weights[0].shape, BF),
            pltpu.VMEM((CHUNK_SLOTS, wide, 2 * mlp), BF),
            pltpu.VMEM(weights[4].shape, BF),
            pltpu.VMEM((n_x, mlp, 2 * wide), BF),
            pltpu.VMEM((rows, n_vis, hd), BF), pltpu.VMEM((rows, n_vis, hd), BF),
            pltpu.VMEM((rows, wide), BF),
            pltpu.VMEM((n_sp - 1, rows, part.shape[1]), F32),
            pltpu.VMEM((n_tp, rows, wide), F32), pltpu.VMEM((peers, rows, wide), F32),
            pltpu.VMEM((2, rows, wide), F32),
            pltpu.VMEM((peers, rows, wide), F32),
            pltpu.VMEM((2, rows, LANES), F32), pltpu.VMEM((peers, rows, LANES), F32),
            pltpu.VMEM((rows, 2 * mlp), F32),
            pltpu.VMEM((rows, mlp), BF),
            pltpu.VMEM((rows, heads * hd), BF),
            pltpu.VMEM((heads, rows, hd), F32),
            pltpu.VMEM((2, n_sp, n_x, rows, wide), F32),
            pltpu.VMEM(part.shape, F32), pltpu.VMEM((3,) + gains[0].shape, BF),
            pltpu.VMEM((3, n_tp, wide // LANES, LANES), F32), pltpu.VMEM(qnorm.shape, BF),
            pltpu.VMEM((rows, n_vis), jnp.int32), dma((6,)),
            dma, dma((CHUNK_SLOTS, 2)), dma, dma((n_x,)), dma((2,)), dma,
            dma((n_sp - 1,)), dma((n_sp - 1,)), dma((peers + 1,)), dma((peers,)), dma((peers,)), dma((peers,)),
            dma((peers,)), dma((peers,)),
            dma((2, 3)), dma((2, 3)), dma((2, 4, 3)), dma((2, 4, 3)), dma((31,)), dma((31,)),
        ],
        compiler_params=pltpu.CompilerParams(collective_id=1, has_side_effects=True, vmem_limit_bytes=67043328),
        name="decode_step",
    )(mask, gates, part, *gains, qnorm, xvalid, hid, *weights, kc, vc)


def solution(mesh):
    cache_spec = P('dp', 'sp', 'tp', None)
    cross_spec = P('dp', None, 'tp', None)
    row_spec = P('dp', None)
    vec_spec = P('dp')
    full_spec = P(None)
    col_spec = P(None, 'tp')
    split_rows = P('tp', None)
    in_specs = (row_spec, vec_spec, cache_spec, cache_spec, cross_spec, cross_spec, row_spec, vec_spec,
                full_spec, col_spec, col_spec, col_spec, split_rows, full_spec, col_spec, col_spec, split_rows,
                full_spec, col_spec, full_spec, split_rows, full_spec, full_spec, col_spec, col_spec, split_rows)
    out_specs = (row_spec, cache_spec, cache_spec)
    n_sp = mesh.shape['sp']
    n_tp = mesh.shape['tp']

    def local_step(hidden, new_pos, k_self, v_self, k_cross, v_cross, xvalid, rowmask,
                   self_attn_norm, self_wq, self_wk, self_wv, self_wo, self_mlp_norm,
                   self_wgate, self_wup, self_wdown, cross_attn_norm, cross_wq, cross_qnorm,
                   cross_wo, cross_gates, cross_mlp_norm, cross_wgate, cross_wup, cross_wdown):
        batch_rows = hidden.shape[0]
        len_local = k_self.shape[1]
        head_dim = k_self.shape[3]
        heads = self_wq.shape[1] // head_dim
        scale = head_dim ** -0.5
        flat = (batch_rows, len_local, head_dim)
        lanes = (-1, LANES)
        part, ko, vo = self_phase(new_pos, hidden, self_attn_norm.reshape(lanes), self_wq, self_wk, self_wv,
                                  k_self.reshape(flat), v_self.reshape(flat), scale=scale)
        gains = tuple(g.reshape(lanes) for g in (self_mlp_norm, cross_attn_norm, cross_mlp_norm))
        weights = (self_wo, self_wgate, self_wup, self_wdown, cross_wq, cross_wo, cross_wgate, cross_wup, cross_wdown)
        cflat = (batch_rows, k_cross.shape[1], head_dim)
        h4 = step_phase(rowmask, cross_gates, part, gains, cross_qnorm.reshape(lanes), xvalid,
                        hidden, weights, k_cross.reshape(cflat), v_cross.reshape(cflat),
                        n_sp=n_sp, n_tp=n_tp, heads=heads, scale=scale)
        return h4, ko.reshape(k_self.shape), vo.reshape(v_self.shape)

    return jax.shard_map(local_step, mesh=mesh, in_specs=in_specs, out_specs=out_specs, check_vma=False)
```

```python
import functools
import math
import jax
import jax.numpy as jnp
import numpy as np
from jax import lax
from jax.experimental import pallas as pl
from jax.experimental.pallas import tpu as pltpu
from jax.sharding import PartitionSpec as P

NORM_EPS = 1e-5
ROPE_THETA = 500000.0
ROPE_FACTOR = 8.0
LOW_FREQ = 1.0
HIGH_FREQ = 4.0
ORIG_CTX = 8192.0
NEG_BIG = -1e30
MESH = pl.DeviceIdType.MESH
BF = jnp.bfloat16
F32 = jnp.float32
LANES = 128
GROUP_ROWS = 8
CHUNK_SLOTS = 6
NT_DIMS = (((1,), (1,)), ((), ()))
ORDER = ((0, 0), (0, 1), (1, 0), (3, 0), (1, 1), (3, 1), (2, 0), (2, 1))
FROM = (0, 1, 3, 2, 5, 4, 6, 7)
CHIPS = (2, 1, 3, 0)


def rope_table(head_dim):
    inv_freq = (1.0 / (ROPE_THETA ** (np.arange(0, head_dim, 2) / head_dim))).astype(np.float32)
    wavelen = 2.0 * math.pi / inv_freq
    smooth = (ORIG_CTX / wavelen - LOW_FREQ) / (HIGH_FREQ - LOW_FREQ)
    mid_freq = (1.0 - smooth) * inv_freq / ROPE_FACTOR + smooth * inv_freq
    scaled = np.where(wavelen > ORIG_CTX / LOW_FREQ, inv_freq / ROPE_FACTOR, mid_freq)
    freqs = np.where(wavelen < ORIG_CTX / HIGH_FREQ, inv_freq, scaled)
    table = np.zeros((8, head_dim), np.float32)
    table[0] = np.concatenate([freqs, freqs])
    table[1] = np.where(np.arange(head_dim) < head_dim // 2, -1.0, 1.0)
    return jnp.asarray(table)


def self_kernel(pos_sm, freq_hbm, hid_hbm, g_hbm, wq_hbm, wk_hbm, wv_hbm, ks_hbm, vs_hbm,
                part_b, ko_hbm, vo_hbm,
                freq_b, hid_b, g_b, xb, w_b, wk_b, wv_b, kb, vb, q_s, kn_s, vn_s, lp_s, s_s,
                i_sem, w_sem, c_sem, o_sem, *, chunks, heads, scale):
    rows, hidden = hid_b.shape
    hd = LANES
    tlen = kb.shape[0] // rows
    kc = hidden // chunks
    qw = heads * hd
    small = [pltpu.make_async_copy(hid_hbm, hid_b, i_sem.at[0]), pltpu.make_async_copy(g_hbm, g_b, i_sem.at[1]),
             pltpu.make_async_copy(freq_hbm, freq_b, i_sem.at[2])]
    for cp in small:
        cp.start()
    kv_in = [pltpu.make_async_copy(wk_hbm, wk_b, i_sem.at[3]), pltpu.make_async_copy(wv_hbm, wv_b, i_sem.at[4]),
             pltpu.make_async_copy(ks_hbm, kb, c_sem.at[0]), pltpu.make_async_copy(vs_hbm, vb, c_sem.at[1])]
    for cp in kv_in:
        cp.start()
    loads = []
    for i in range(chunks):
        sl = pl.ds(i * kc, kc)
        loads.append(pltpu.make_async_copy(wq_hbm.at[sl], w_b.at[sl], w_sem.at[i]))
        loads[-1].start()
    for cp in small:
        cp.wait()
    acc = jnp.zeros((rows, LANES), F32)
    for c in range(hidden // LANES):
        v = hid_b[:, c * LANES:(c + 1) * LANES].astype(F32)
        acc = acc + v * v
    inv = lax.rsqrt(jnp.sum(acc, axis=-1, keepdims=True) * (1.0 / hidden) + NORM_EPS)
    g_all = g_b[...].astype(F32)
    for c in range(hidden // LANES):
        sl = slice(c * LANES, (c + 1) * LANES)
        xb[:, sl] = (hid_b[:, sl].astype(F32) * inv * g_all[c:c + 1, :]).astype(BF)
    gr = GROUP_ROWS
    sub = lax.broadcasted_iota(jnp.int32, (gr, LANES), 0)
    pos_rows = []
    for g in range(rows // gr):
        pg = jnp.zeros((gr, LANES), jnp.int32)
        for i in range(gr):
            pg = jnp.where(sub == i, pos_sm[g * gr + i], pg)
        pos_rows.append(pg)
    pos_v = jnp.concatenate(pos_rows, axis=0)
    first = lax.axis_index("sp") * tlen
    lp_s[...] = pos_v - first
    ang = pos_v.astype(F32) * freq_b[0:1, :]
    cos_t = jnp.cos(ang)
    sin_t = jnp.sin(ang) * freq_b[1:2, :]

    def rope(v):
        v = v.astype(BF).astype(F32)
        return (v * cos_t + pltpu.roll(v, hd // 2, 1) * sin_t).astype(BF).astype(F32)

    for cp in kv_in:
        cp.wait()
    kn_s[...] = rope(jnp.dot(xb[...], wk_b[...], preferred_element_type=F32))
    vn_s[...] = jnp.dot(xb[...], wv_b[...], preferred_element_type=F32).astype(BF).astype(F32)
    span = gr * tlen
    t_iota = lax.broadcasted_iota(jnp.int32, (tlen, hd), 0)

    def update(g, carry):
        base = pl.multiple_of(g * gr, gr)
        for i in range(gr):
            hit = t_iota == pos_sm[base + i] - first
            sl = pl.ds(pl.multiple_of((base + i) * tlen, tlen), tlen)
            kb[sl, :] = jnp.where(hit, kn_s[pl.ds(base + i, 1), :], kb[sl, :].astype(F32)).astype(BF)
            vb[sl, :] = jnp.where(hit, vn_s[pl.ds(base + i, 1), :], vb[sl, :].astype(F32)).astype(BF)
        return carry

    lax.fori_loop(0, rows // gr, update, 0)
    k_out = pltpu.make_async_copy(kb, ko_hbm, o_sem.at[0])
    v_out = pltpu.make_async_copy(vb, vo_hbm, o_sem.at[1])
    k_out.start()
    v_out.start()
    qq = None
    for i in range(chunks):
        loads[i].wait()
        part = jnp.dot(xb[:, i * kc:(i + 1) * kc], w_b[i * kc:(i + 1) * kc, :], preferred_element_type=F32)
        qq = part if qq is None else qq + part
    for h in range(heads):
        q_s[h] = rope(qq[:, h * hd:(h + 1) * hd])
    groups = rows // gr
    for g in range(groups):
        rs = slice(g * gr, (g + 1) * gr)
        qg = jnp.concatenate([q_s[h, rs, :] for h in range(heads)], axis=0).astype(BF)
        s_s[g] = lax.dot_general(qg, kb[g * span:(g + 1) * span, :], NT_DIMS, preferred_element_type=F32)
    col = lax.broadcasted_iota(jnp.int32, (heads * gr, LANES), 1)
    row = lax.broadcasted_iota(jnp.int32, (heads * gr, LANES), 0)
    lane = lax.broadcasted_iota(jnp.int32, (gr, LANES), 1)
    tcol = col % tlen
    for g in range(groups):
        rs = slice(g * gr, (g + 1) * gr)
        lp = jnp.concatenate([lp_s[rs, :]] * heads, axis=0)
        seen = tcol <= lp
        oks, ss = [], []
        for c in range(span // LANES):
            ok = jnp.logical_and(seen, c * (LANES // tlen) + col // tlen == row % gr)
            oks.append(ok)
            ss.append(jnp.where(ok, s_s[g, :, c * LANES:(c + 1) * LANES] * scale, NEG_BIG))
        m = jnp.max(functools.reduce(jnp.maximum, ss), axis=-1, keepdims=True)
        ps = [jnp.where(ok, jnp.exp(s - m), 0.0) for ok, s in zip(oks, ss)]
        l = jnp.sum(functools.reduce(jnp.add, ps), axis=-1, keepdims=True)
        p = jnp.concatenate(ps, axis=1).astype(BF)
        o = jnp.dot(p, vb[g * span:(g + 1) * span, :], preferred_element_type=F32)
        stat = jnp.zeros((gr, LANES), F32)
        for h in range(heads):
            hs = slice(h * gr, (h + 1) * gr)
            part_b[rs, h * hd:(h + 1) * hd] = o[hs]
            stat = jnp.where(lane == h, m[hs], stat)
            stat = jnp.where(lane == heads + h, l[hs], stat)
        part_b[rs, qw:] = stat
    k_out.wait()
    v_out.wait()


def self_phase(pos, hid, gain, wq, wk, wv, ks, vs, *, scale):
    rows, hidden = hid.shape
    tlen = ks.shape[1]
    hd = ks.shape[2]
    heads = wq.shape[1] // hd
    chunks = 4
    ks = ks.reshape(rows * tlen, hd)
    vs = vs.reshape(rows * tlen, hd)
    freq = rope_table(hd)
    anys = pl.BlockSpec(memory_space=pl.ANY)
    cache = jax.ShapeDtypeStruct(ks.shape, BF)
    pshape = (rows, heads * hd + LANES)
    return pl.pallas_call(
        functools.partial(self_kernel, chunks=chunks, heads=heads, scale=scale),
        out_shape=(jax.ShapeDtypeStruct(pshape, F32), cache, cache),
        in_specs=[pl.BlockSpec(memory_space=pltpu.SMEM)] + [anys] * 8,
        out_specs=(pl.BlockSpec(memory_space=pltpu.VMEM), anys, anys),
        scratch_shapes=[
            pltpu.VMEM(freq.shape, F32), pltpu.VMEM((rows, hidden), BF), pltpu.VMEM(gain.shape, BF),
            pltpu.VMEM((rows, hidden), BF), pltpu.VMEM(wq.shape, BF),
            pltpu.VMEM(wk.shape, BF), pltpu.VMEM(wv.shape, BF),
            pltpu.VMEM(ks.shape, BF), pltpu.VMEM(vs.shape, BF),
            pltpu.VMEM((heads, rows, hd), F32), pltpu.VMEM((rows, hd), F32), pltpu.VMEM((rows, hd), F32),
            pltpu.VMEM((rows, LANES), jnp.int32),
            pltpu.VMEM((rows // GROUP_ROWS, heads * GROUP_ROWS, GROUP_ROWS * tlen), F32),
            pltpu.SemaphoreType.DMA((5,)), pltpu.SemaphoreType.DMA((chunks,)), pltpu.SemaphoreType.DMA((2,)),
            pltpu.SemaphoreType.DMA((2,)),
        ],
        compiler_params=pltpu.CompilerParams(vmem_limit_bytes=60 << 20),
        name="self_attention",
    )(pos, freq, hid, gain, wq, wk, wv, ks, vs)


def step_kernel(mask_sm, gate_sm, part_b, g2_hbm, g3_hbm, g4_hbm, qn_hbm, xv_hbm,
                hid_hbm, wo_hbm, wg_hbm, wu_hbm, wd_hbm, wqc_hbm, woc_hbm, wgc_hbm, wuc_hbm, wdc_hbm, kc_hbm, vc_hbm,
                out_ref,
                wo_b, chunk_b, qc_b, down_b, kc_b, vc_b, hid_b, comb, sbuf, rbuf, piece, full, stat, stats, acc_s, act, ob,
                fin, gain_b, gain_f, qn_ref, xv_ref, small_sem,
                wo_sem, chunk_sem, qc_sem, down_sem, kv_sem, hid_sem, cs_sem, cr_sem, rs_ssem, rs_rsem, ag_ssem, ag_rsem,
                st_ssem, st_rsem, fd_ssem, fd_rsem, ff_ssem, ff_rsem, fc_ssem, fc_rsem, *, n_sp, n_tp, heads, scale):
    sp = lax.axis_index("sp")
    tp = lax.axis_index("tp")
    xx = tp // 2
    cc = tp % 2
    n_x = n_tp // 2
    rows = hid_b.shape[0]
    wide = hid_b.shape[1]
    mlp = act.shape[1]
    hd = LANES
    gr = GROUP_ROWS
    per = wide // LANES
    r0 = pl.multiple_of(sp * rows, rows)

    def tp_at(k):
        dx, dc = ORDER[k]
        return ((xx + dx) % n_x) * 2 + (cc + dc) % 2

    def remote(src, dst, ssem, rsem, **dev):
        return pltpu.make_async_remote_copy(src_ref=src, dst_ref=dst, send_sem=ssem, recv_sem=rsem,
                                            device_id=dev, device_id_type=MESH)

    bar = pltpu.get_barrier_semaphore()
    for j in range(1, n_sp):
        pl.semaphore_signal(bar, inc=1, device_id={"sp": (sp + j) % n_sp}, device_id_type=MESH)
    for k in range(1, n_tp):
        pl.semaphore_signal(bar, inc=1, device_id={"tp": tp_at(k)}, device_id_type=MESH)

    def chunk_copies(n):
        slot = n % CHUNK_SLOTS
        a, b = ((wg_hbm, wu_hbm), (wgc_hbm, wuc_hbm))[n // n_tp]
        src = pl.ds(pl.multiple_of(tp_at(n % n_tp) * wide, wide), wide)
        return [pltpu.make_async_copy(a.at[src], chunk_b.at[slot, :, pl.ds(0, mlp)], chunk_sem.at[slot, 0]),
                pltpu.make_async_copy(b.at[src], chunk_b.at[slot, :, pl.ds(mlp, mlp)], chunk_sem.at[slot, 1])]

    def start_chunks(first, last):
        for n in range(first, last):
            for cp in chunk_copies(n):
                cp.start()

    def chip_at(i):
        return (xx + CHIPS[i]) % n_x

    def down_copy(layer, i):
        src = (wd_hbm, wdc_hbm)[layer]
        return pltpu.make_async_copy(src.at[:, pl.ds(pl.multiple_of(chip_at(i) * 2 * wide, LANES), 2 * wide)],
                                     down_b.at[i], down_sem.at[i])

    wo_copy = pltpu.make_async_copy(wo_hbm, wo_b, wo_sem)
    woc_copy = pltpu.make_async_copy(woc_hbm, wo_b, wo_sem)
    qc_copy = pltpu.make_async_copy(wqc_hbm, qc_b, qc_sem)
    hid_copy = pltpu.make_async_copy(
        hid_hbm.at[pl.ds(r0, rows), pl.ds(pl.multiple_of(tp * wide, LANES), wide)], hid_b, hid_sem)
    kc_copy = pltpu.make_async_copy(kc_hbm.at[pl.ds(r0, rows)], kc_b, kv_sem.at[0])
    vc_copy = pltpu.make_async_copy(vc_hbm.at[pl.ds(r0, rows)], vc_b, kv_sem.at[1])
    small = [pltpu.make_async_copy(g2_hbm, gain_b.at[0], small_sem.at[1]),
             pltpu.make_async_copy(g3_hbm, gain_b.at[1], small_sem.at[2]),
             pltpu.make_async_copy(g4_hbm, gain_b.at[2], small_sem.at[3]),
             pltpu.make_async_copy(qn_hbm, qn_ref, small_sem.at[4]),
             pltpu.make_async_copy(xv_hbm.at[pl.ds(r0, rows)], xv_ref, small_sem.at[5])]
    for cp in small:
        cp.start()
    wo_copy.start()
    hid_copy.start()
    start_chunks(0, 3)
    pl.semaphore_wait(bar, n_sp - 1 + n_tp - 1)

    sends = []
    for i, j in enumerate((2, 1, 3)):
        peer = (sp + j) % n_sp
        cp = remote(part_b.at[pl.ds(pl.multiple_of(peer * rows, rows), rows)], comb.at[i],
                    cs_sem.at[i], cr_sem.at[i], sp=peer)
        cp.start()
        sends.append(cp)
    start_chunks(3, CHUNK_SLOTS)
    for cp in small:
        cp.wait()
    for i in range(3):
        g_all = gain_b[i].astype(F32)
        for j in range(n_tp):
            gain_f[i, j] = g_all[j * per:(j + 1) * per, :]
    for cp in sends:
        cp.wait()
    qw = heads * hd
    own = part_b[pl.ds(r0, rows), :]
    blocks = [own] + [comb[j] for j in range(n_sp - 1)]
    for h in range(heads):
        ms = [b[:, qw + h:qw + h + 1] for b in blocks]
        top = functools.reduce(jnp.maximum, ms)
        fs = [jnp.exp(m - top) for m in ms]
        den = sum(b[:, qw + heads + h:qw + heads + h + 1] * f for b, f in zip(blocks, fs))
        num = sum(b[:, h * hd:(h + 1) * hd] * f for b, f in zip(blocks, fs))
        ob[:, h * hd:(h + 1) * hd] = (num / den).astype(BF)

    whole = ((0, 0, rows),)
    halves = ((0, 0, rows // 2), (1, rows // 2, rows // 2))
    last = 2 * (n_x - 1)

    def reduce_send(product, parts):
        sent = []
        for i in range(n_x):
            out = product(i)
            lo = parts[0][1]
            n = out.shape[0]
            sbuf[2 * i, lo:lo + n] = out[:, :wide]
            sbuf[2 * i + 1, lo:lo + n] = out[:, wide:]
            if i < n_x - 1:
                for h, r, n in parts:
                    for c in range(2):
                        cp = remote(sbuf.at[2 * i + c, pl.ds(r, n)], rbuf.at[2 * i + cc, pl.ds(r, n)],
                                    rs_ssem.at[h, 2 * i + c], rs_rsem.at[h, 2 * i + cc], tp=chip_at(i) * 2 + c)
                        cp.start()
                        sent.append(cp)
        for h, r, n in parts:
            cp = remote(sbuf.at[last + 1 - cc, pl.ds(r, n)], rbuf.at[last, pl.ds(r, n)], rs_ssem.at[h, last],
                        rs_rsem.at[h, last], tp=xx * 2 + 1 - cc)
            cp.start()
            sent.append(cp)
        return sent

    def reduce_wait(part):
        h, r, n = part
        acc = sbuf[last + cc, r:r + n]
        for j in (6, 2, 3, 4, 5, 0, 1):
            remote(sbuf.at[j, pl.ds(r, n)], rbuf.at[j, pl.ds(r, n)], rs_ssem.at[h, j], rs_rsem.at[h, j],
                   tp=xx * 2 + 1 - cc).wait_recv()
            acc = acc + rbuf[j, r:r + n]
        return acc

    def done(sent):
        for cp in sent:
            cp.wait_send()

    def reduce_scatter(product, then=None):
        sent = reduce_send(product, whole)
        if then is not None:
            then()
        acc = reduce_wait(whole[0])
        done(sent)
        return acc

    def share_send(cur, slot, part):
        h, r, n = part
        rs = pl.ds(r, n)
        piece[slot, r:r + n] = cur
        stat[slot, r:r + n] = jnp.broadcast_to(jnp.sum(cur * cur, axis=-1, keepdims=True), (n, LANES))
        sent = []
        for k in range(1, n_tp):
            cp = remote(stat.at[slot, rs], stats.at[k - 1, rs], st_ssem.at[h, k - 1], st_rsem.at[h, k - 1], tp=tp_at(k))
            cp.start()
            sent.append(cp)
        for k in range(1, n_tp):
            cp = remote(piece.at[slot, rs], full.at[k - 1, rs], ag_ssem.at[h, k - 1], ag_rsem.at[h, k - 1], tp=tp_at(k))
            cp.start()
            sent.append(cp)
        return sent

    def share_use(cur, slot, part, gain, use):
        h, r, n = part
        rs = pl.ds(r, n)
        tot = stat[slot, r:r + n]
        for k in range(1, n_tp):
            remote(stat.at[slot, rs], stats.at[k - 1, rs], st_ssem.at[h, k - 1], st_rsem.at[h, k - 1],
                   tp=tp_at(k)).wait_recv()
            tot = tot + stats[k - 1, r:r + n]
        inv = lax.rsqrt(tot * (1.0 / (n_tp * wide)) + NORM_EPS)
        for k in range(n_tp):
            if k == 0:
                v = cur
            else:
                j = FROM[k] - 1
                remote(piece.at[slot, rs], full.at[j, rs], ag_ssem.at[h, j], ag_rsem.at[h, j], tp=tp_at(k)).wait_recv()
                v = full[j, r:r + n]
            g = gain_f[gain, tp_at(k)]
            x = [v[:, i * LANES:(i + 1) * LANES] * inv * g[i:i + 1, :] for i in range(per)]
            use(k, jnp.concatenate(x, axis=1).astype(BF))

    def gate_up(layer, cur, slot, gain):
        def use(k, x):
            n = layer * n_tp + k
            for cp in chunk_copies(n):
                cp.wait()
            out = jnp.dot(x, chunk_b[n % CHUNK_SLOTS], preferred_element_type=F32)
            if k == 0:
                acc_s[...] = out
            else:
                acc_s[...] += out
            if k + CHUNK_SLOTS < n_tp:
                start_chunks(n + CHUNK_SLOTS, n + CHUNK_SLOTS + 1)

        sent = share_send(cur, slot, whole[0])
        share_use(cur, slot, whole[0], gain, use)
        done(sent)
        gate = acc_s[:, :mlp].astype(BF).astype(F32)
        up = acc_s[:, mlp:].astype(BF).astype(F32)
        act[...] = (gate * jax.nn.sigmoid(gate) * up).astype(BF)

    def load_down(layer):
        for i in range(n_x):
            down_copy(layer, i).start()

    def load_cross_mlp():
        start_chunks(n_tp, n_tp + CHUNK_SLOTS)
        load_down(1)

    def down(layer):
        def product(i):
            down_copy(layer, i).wait()
            return jnp.dot(act[...], down_b[i], preferred_element_type=F32)

        return product

    def wo_product(i, r=0, n=rows):
        return jnp.dot(ob[r:r + n, :], wo_b[:, pl.ds(pl.multiple_of(chip_at(i) * 2 * wide, LANES), 2 * wide)],
                       preferred_element_type=F32)

    def rounded(v):
        return v.astype(BF).astype(F32)

    def row_scale(i):
        sub = lax.broadcasted_iota(jnp.int32, (rows, LANES), 0)
        out = jnp.zeros((rows, LANES), jnp.int32)
        for r in range(rows):
            out = jnp.where(sub == r, mask_sm[r0 + r], out)
        return (jnp.tanh(jnp.full((rows, LANES), gate_sm[i], F32)) * out.astype(F32))[:, 0:1]

    wo_copy.wait()
    acc = reduce_scatter(wo_product, lambda: load_down(0))
    hid_copy.wait()
    gate_up(0, rounded(hid_b[...].astype(F32) + acc), 0, 0)
    woc_copy.start()
    qc_copy.start()
    kc_copy.start()
    vc_copy.start()
    sent_d = reduce_send(down(0), halves)
    load_cross_mlp()

    cur, sent_g = [], []
    for part in halves:
        h, r, n = part
        cur.append(rounded(piece[0, r:r + n] + reduce_wait(part)))
        sent_g += share_send(cur[h], 1, part)
    done(sent_d)
    qc_copy.wait()
    kc_copy.wait()
    vc_copy.wait()
    woc_copy.wait()
    n_vis = kc_b.shape[1]
    rmod = lax.broadcasted_iota(jnp.int32, (heads * gr, n_vis), 0) % gr
    sent_o = []
    for part in halves:
        g, r, _ = part
        q_parts = []

        def use_q(k, x):
            w = qc_b[pl.ds(pl.multiple_of(tp_at(k) * wide, wide), wide), :]
            out = jnp.dot(x, w, preferred_element_type=F32)
            q_parts[:] = [out if k == 0 else q_parts[0] + out]

        share_use(cur[g], 1, part, 1, use_q)
        qs = []
        for h in range(heads):
            v = rounded(q_parts[0][:, h * hd:(h + 1) * hd])
            inv = lax.rsqrt(jnp.mean(v * v, axis=-1, keepdims=True) + NORM_EPS)
            qs.append(rounded(v * inv * qn_ref[...].astype(F32)))
        qg = jnp.concatenate(qs, axis=0).astype(BF)
        s = jnp.zeros((heads * gr, n_vis), F32)
        for i in range(gr):
            s_i = lax.dot_general(qg, kc_b[r + i], NT_DIMS, preferred_element_type=F32)
            s = jnp.where(rmod == i, s_i, s)
        valid = xv_ref[r:r + gr, :]
        ok = jnp.concatenate([valid] * heads, axis=0) > 0
        s = jnp.where(ok, s * scale, NEG_BIG)
        m = jnp.max(s, axis=-1, keepdims=True)
        pr = jnp.where(ok, jnp.exp(s - m), 0.0)
        l = jnp.sum(pr, axis=-1, keepdims=True)
        o = jnp.zeros((heads * gr, hd), F32)
        for i in range(gr):
            o = o + jnp.dot(jnp.where(rmod == i, pr, 0.0).astype(BF), vc_b[r + i], preferred_element_type=F32)
        o = o / l
        for h in range(heads):
            ob[r:r + gr, h * hd:(h + 1) * hd] = o[h * gr:(h + 1) * gr].astype(BF)
        sent_o += reduce_send(functools.partial(wo_product, r=r, n=gr), (part,))
    done(sent_g)
    acc = jnp.concatenate([reduce_wait(part) for part in halves], axis=0)
    done(sent_o)

    gate_up(1, rounded(piece[1] + row_scale(0) * acc), 0, 2)
    acc = reduce_scatter(down(1))
    fin[cc, sp, xx] = rounded(piece[0] + row_scale(1) * acc)

    half = rows // 2
    top = pl.ds(0, half)
    bot = pl.ds(half, half)

    def hop_x(src_sp, src_x, part, dx, ssem, rsem):
        blk = fin.at[cc, src_sp, src_x, part]
        return remote(blk, blk, ssem, rsem, tp=((xx + dx) % n_x) * 2 + cc)

    def hop_y(src_sp, src_x, part, dy, ssem, rsem):
        blk = fin.at[cc, src_sp, src_x, part]
        return remote(blk, blk, ssem, rsem, sp=(sp + dy) % n_sp)

    across = []

    def hop_core(src_sp, src_x, *part):
        blk = fin.at[(cc, src_sp, src_x) + part]
        i = len(across)
        cp = remote(blk, blk, fc_ssem.at[i], fc_rsem.at[i], tp=xx * 2 + (1 - cc))
        cp.start()
        across.append(cp)

    steps = (2, 1, 3)
    first = []
    for i, d in enumerate(steps):
        cx = hop_x(sp, xx, top, d, fd_ssem.at[0, i], fd_rsem.at[0, i])
        cy = hop_y(sp, xx, bot, d, fd_ssem.at[1, i], fd_rsem.at[1, i])
        cx.start()
        cy.start()
        first.append((cx, cy))
    second = []

    def forward(a, from_x, from_y):
        for i, d in enumerate(steps):
            cy = hop_y(sp, from_x, top, d, ff_ssem.at[0, a, i], ff_rsem.at[0, a, i])
            cx = hop_x(from_y, xx, bot, d, ff_ssem.at[1, a, i], ff_rsem.at[1, a, i])
            cy.start()
            cx.start()
            second.append((cx, from_y, (xx + n_x - d) % n_x, cy, (sp + n_sp - d) % n_sp, from_x))

    forward(0, xx, sp)
    hop_core(sp, xx)
    for a, i in ((1, 1), (2, 2), (3, 0)):
        cx, cy = first[i]
        from_x = (xx + n_x - steps[i]) % n_x
        from_y = (sp + n_sp - steps[i]) % n_sp
        cx.wait_recv()
        cy.wait_recv()
        forward(a, from_x, from_y)
        hop_core(sp, from_x, top)
        hop_core(from_y, xx, bot)
    for cx, b_sp, b_x, cy, t_sp, t_x in second:
        cx.wait_recv()
        hop_core(b_sp, b_x, bot)
        cy.wait_recv()
        hop_core(t_sp, t_x, top)
    for cx, cy in first:
        cx.wait_send()
        cy.wait_send()
    for cx, _, _, cy, _, _ in second:
        cx.wait_send()
        cy.wait_send()
    for cp in across:
        cp.wait()
    for c in range(2):
        for s in range(n_sp):
            for x in range(n_x):
                j = x * 2 + c
                out_ref[s * rows:(s + 1) * rows, j * wide:(j + 1) * wide] = fin[c, s, x].astype(BF)


def step_phase(mask, gates, part, gains, qnorm, xvalid, hid, weights, kc, vc, *, n_sp, n_tp, heads, scale):
    all_rows, hidden = hid.shape
    rows = all_rows // n_sp
    wide = hidden // n_tp
    mlp = weights[1].shape[1]
    n_vis, hd = kc.shape[1], kc.shape[2]
    vm = pl.BlockSpec(memory_space=pltpu.VMEM)
    anys = pl.BlockSpec(memory_space=pl.ANY)
    dma = pltpu.SemaphoreType.DMA
    n_x = n_tp // 2
    peers = n_tp - 1
    pwide = part.shape[1]
    return pl.pallas_call(
        functools.partial(step_kernel, n_sp=n_sp, n_tp=n_tp, heads=heads, scale=scale),
        out_shape=jax.ShapeDtypeStruct((all_rows, hidden), BF),
        in_specs=[pl.BlockSpec(memory_space=pltpu.SMEM)] * 2 + [vm] + [anys] * 17,
        out_specs=vm,
        scratch_shapes=[
            pltpu.VMEM(weights[0].shape, BF),
            pltpu.VMEM((CHUNK_SLOTS, wide, 2 * mlp), BF),
            pltpu.VMEM(weights[4].shape, BF),
            pltpu.VMEM((n_x, mlp, 2 * wide), BF),
            pltpu.VMEM((rows, n_vis, hd), BF), pltpu.VMEM((rows, n_vis, hd), BF),
            pltpu.VMEM((rows, wide), BF),
            pltpu.VMEM((n_sp - 1, rows, pwide), F32),
            pltpu.VMEM((n_tp, rows, wide), F32), pltpu.VMEM((peers, rows, wide), F32),
            pltpu.VMEM((2, rows, wide), F32),
            pltpu.VMEM((peers, rows, wide), F32),
            pltpu.VMEM((2, rows, LANES), F32), pltpu.VMEM((peers, rows, LANES), F32),
            pltpu.VMEM((rows, 2 * mlp), F32),
            pltpu.VMEM((rows, mlp), BF),
            pltpu.VMEM((rows, heads * hd), BF),
            pltpu.VMEM((2, n_sp, n_x, rows, wide), F32),
            pltpu.VMEM((3,) + gains[0].shape, BF),
            pltpu.VMEM((3, n_tp, wide // LANES, LANES), F32), pltpu.VMEM(qnorm.shape, BF),
            pltpu.VMEM((rows, n_vis), jnp.int32), dma((6,)),
            dma, dma((CHUNK_SLOTS, 2)), dma, dma((n_x,)), dma((2,)), dma,
            dma((n_sp - 1,)), dma((n_sp - 1,)), dma((2, peers)), dma((2, peers)), dma((2, peers)), dma((2, peers)),
            dma((2, peers)), dma((2, peers)),
            dma((2, 3)), dma((2, 3)), dma((2, 4, 3)), dma((2, 4, 3)), dma((31,)), dma((31,)),
        ],
        compiler_params=pltpu.CompilerParams(collective_id=1, has_side_effects=True, vmem_limit_bytes=67043328),
        name="decode_step",
    )(mask, gates, part, *gains, qnorm, xvalid, hid, *weights, kc, vc)


def solution(mesh):
    cache_spec = P('dp', 'sp', 'tp', None)
    cross_spec = P('dp', None, 'tp', None)
    row_spec = P('dp', None)
    vec_spec = P('dp')
    full_spec = P(None)
    col_spec = P(None, 'tp')
    split_rows = P('tp', None)
    in_specs = (row_spec, vec_spec, cache_spec, cache_spec, cross_spec, cross_spec, row_spec, vec_spec,
                full_spec, col_spec, col_spec, col_spec, split_rows, full_spec, col_spec, col_spec, split_rows,
                full_spec, col_spec, full_spec, split_rows, full_spec, full_spec, col_spec, col_spec, split_rows)
    out_specs = (row_spec, cache_spec, cache_spec)
    n_sp = mesh.shape['sp']
    n_tp = mesh.shape['tp']

    def local_step(hidden, new_pos, k_self, v_self, k_cross, v_cross, xvalid, rowmask,
                   self_attn_norm, self_wq, self_wk, self_wv, self_wo, self_mlp_norm,
                   self_wgate, self_wup, self_wdown, cross_attn_norm, cross_wq, cross_qnorm,
                   cross_wo, cross_gates, cross_mlp_norm, cross_wgate, cross_wup, cross_wdown):
        batch_rows = hidden.shape[0]
        len_local = k_self.shape[1]
        head_dim = k_self.shape[3]
        heads = self_wq.shape[1] // head_dim
        scale = head_dim ** -0.5
        flat = (batch_rows, len_local, head_dim)
        lanes = (-1, LANES)
        part, ko, vo = self_phase(new_pos, hidden, self_attn_norm.reshape(lanes), self_wq, self_wk, self_wv,
                                  k_self.reshape(flat), v_self.reshape(flat), scale=scale)
        gains = tuple(g.reshape(lanes) for g in (self_mlp_norm, cross_attn_norm, cross_mlp_norm))
        weights = (self_wo, self_wgate, self_wup, self_wdown, cross_wq, cross_wo, cross_wgate, cross_wup, cross_wdown)
        cflat = (batch_rows, k_cross.shape[1], head_dim)
        h4 = step_phase(rowmask, cross_gates, part, gains, cross_qnorm.reshape(lanes), xvalid,
                        hidden, weights, k_cross.reshape(cflat), v_cross.reshape(cflat),
                        n_sp=n_sp, n_tp=n_tp, heads=heads, scale=scale)
        return h4, ko.reshape(k_self.shape), vo.reshape(v_self.shape)

    return jax.shard_map(local_step, mesh=mesh, in_specs=in_specs, out_specs=out_specs, check_vma=False)
```

```python
import functools
import math
import jax
import jax.numpy as jnp
import numpy as np
from jax import lax
from jax.experimental import pallas as pl
from jax.experimental.pallas import tpu as pltpu
from jax.sharding import PartitionSpec as P

NORM_EPS = 1e-5
ROPE_THETA = 500000.0
ROPE_FACTOR = 8.0
LOW_FREQ = 1.0
HIGH_FREQ = 4.0
ORIG_CTX = 8192.0
NEG_BIG = -1e30
MESH = pl.DeviceIdType.MESH
BF = jnp.bfloat16
F32 = jnp.float32
LANES = 128
GROUP_ROWS = 8
CHUNK_SLOTS = 6
NT_DIMS = (((1,), (1,)), ((), ()))
ORDER = ((0, 0), (0, 1), (1, 0), (3, 0), (1, 1), (3, 1), (2, 0), (2, 1))
FROM = (0, 1, 3, 2, 5, 4, 6, 7)
CHIPS = (2, 1, 3, 0)


def rope_table(head_dim):
    inv_freq = (1.0 / (ROPE_THETA ** (np.arange(0, head_dim, 2) / head_dim))).astype(np.float32)
    wavelen = 2.0 * math.pi / inv_freq
    smooth = (ORIG_CTX / wavelen - LOW_FREQ) / (HIGH_FREQ - LOW_FREQ)
    mid_freq = (1.0 - smooth) * inv_freq / ROPE_FACTOR + smooth * inv_freq
    scaled = np.where(wavelen > ORIG_CTX / LOW_FREQ, inv_freq / ROPE_FACTOR, mid_freq)
    freqs = np.where(wavelen < ORIG_CTX / HIGH_FREQ, inv_freq, scaled)
    table = np.zeros((8, head_dim), np.float32)
    table[0] = np.concatenate([freqs, freqs])
    table[1] = np.where(np.arange(head_dim) < head_dim // 2, -1.0, 1.0)
    return jnp.asarray(table)


def self_kernel(pos_sm, freq_hbm, hid_hbm, g_hbm, wq_hbm, wk_hbm, wv_hbm, ks_hbm, vs_hbm,
                part_b, ko_hbm, vo_hbm,
                freq_b, hid_b, g_b, xb, w_b, wk_b, wv_b, kb, vb, q_s, kn_s, vn_s, lp_s, s_s,
                i_sem, w_sem, c_sem, o_sem, *, chunks, heads, scale):
    rows, hidden = hid_b.shape
    hd = LANES
    tlen = kb.shape[0] // rows
    kc = hidden // chunks
    qw = heads * hd
    small = [pltpu.make_async_copy(hid_hbm, hid_b, i_sem.at[0]), pltpu.make_async_copy(g_hbm, g_b, i_sem.at[1]),
             pltpu.make_async_copy(freq_hbm, freq_b, i_sem.at[2])]
    for cp in small:
        cp.start()
    kv_in = [pltpu.make_async_copy(wk_hbm, wk_b, i_sem.at[3]), pltpu.make_async_copy(wv_hbm, wv_b, i_sem.at[4]),
             pltpu.make_async_copy(ks_hbm, kb, c_sem.at[0]), pltpu.make_async_copy(vs_hbm, vb, c_sem.at[1])]
    for cp in kv_in:
        cp.start()
    for cp in small:
        cp.wait()
    acc = jnp.zeros((rows, LANES), F32)
    for c in range(hidden // LANES):
        v = hid_b[:, c * LANES:(c + 1) * LANES].astype(F32)
        acc = acc + v * v
    inv = lax.rsqrt(jnp.sum(acc, axis=-1, keepdims=True) * (1.0 / hidden) + NORM_EPS)
    g_all = g_b[...].astype(F32)
    for c in range(hidden // LANES):
        sl = slice(c * LANES, (c + 1) * LANES)
        xb[:, sl] = (hid_b[:, sl].astype(F32) * inv * g_all[c:c + 1, :]).astype(BF)
    loads = []
    for i in range(chunks):
        sl = pl.ds(i * kc, kc)
        loads.append(pltpu.make_async_copy(wq_hbm.at[sl], w_b.at[sl], w_sem.at[i]))
        loads[-1].start()
    gr = GROUP_ROWS
    sub = lax.broadcasted_iota(jnp.int32, (gr, LANES), 0)
    pos_rows = []
    for g in range(rows // gr):
        pg = jnp.zeros((gr, LANES), jnp.int32)
        for i in range(gr):
            pg = jnp.where(sub == i, pos_sm[g * gr + i], pg)
        pos_rows.append(pg)
    pos_v = jnp.concatenate(pos_rows, axis=0)
    first = lax.axis_index("sp") * tlen
    lp_s[...] = pos_v - first
    ang = pos_v.astype(F32) * freq_b[0:1, :]
    cos_t = jnp.cos(ang)
    sin_t = jnp.sin(ang) * freq_b[1:2, :]

    def rope(v):
        v = v.astype(BF).astype(F32)
        return (v * cos_t + pltpu.roll(v, hd // 2, 1) * sin_t).astype(BF).astype(F32)

    for cp in kv_in:
        cp.wait()
    kn_s[...] = rope(jnp.dot(xb[...], wk_b[...], preferred_element_type=F32))
    vn_s[...] = jnp.dot(xb[...], wv_b[...], preferred_element_type=F32).astype(BF).astype(F32)
    span = gr * tlen
    t_iota = lax.broadcasted_iota(jnp.int32, (tlen, hd), 0)

    def update(g, carry):
        base = pl.multiple_of(g * gr, gr)
        for i in range(gr):
            hit = t_iota == pos_sm[base + i] - first
            sl = pl.ds(pl.multiple_of((base + i) * tlen, tlen), tlen)
            kb[sl, :] = jnp.where(hit, kn_s[pl.ds(base + i, 1), :], kb[sl, :].astype(F32)).astype(BF)
            vb[sl, :] = jnp.where(hit, vn_s[pl.ds(base + i, 1), :], vb[sl, :].astype(F32)).astype(BF)
        return carry

    lax.fori_loop(0, rows // gr, update, 0)
    k_out = pltpu.make_async_copy(kb, ko_hbm, o_sem.at[0])
    v_out = pltpu.make_async_copy(vb, vo_hbm, o_sem.at[1])
    k_out.start()
    v_out.start()
    qq = None
    for i in range(chunks):
        loads[i].wait()
        part = jnp.dot(xb[:, i * kc:(i + 1) * kc], w_b[i * kc:(i + 1) * kc, :], preferred_element_type=F32)
        qq = part if qq is None else qq + part
    for h in range(heads):
        q_s[h] = rope(qq[:, h * hd:(h + 1) * hd])
    groups = rows // gr
    for g in range(groups):
        rs = slice(g * gr, (g + 1) * gr)
        qg = jnp.concatenate([q_s[h, rs, :] for h in range(heads)], axis=0).astype(BF)
        s_s[g] = lax.dot_general(qg, kb[g * span:(g + 1) * span, :], NT_DIMS, preferred_element_type=F32)
    col = lax.broadcasted_iota(jnp.int32, (heads * gr, LANES), 1)
    row = lax.broadcasted_iota(jnp.int32, (heads * gr, LANES), 0)
    lane = lax.broadcasted_iota(jnp.int32, (gr, LANES), 1)
    tcol = col % tlen
    for g in range(groups):
        rs = slice(g * gr, (g + 1) * gr)
        lp = jnp.concatenate([lp_s[rs, :]] * heads, axis=0)
        seen = tcol <= lp
        oks, ss = [], []
        for c in range(span // LANES):
            ok = jnp.logical_and(seen, c * (LANES // tlen) + col // tlen == row % gr)
            oks.append(ok)
            ss.append(jnp.where(ok, s_s[g, :, c * LANES:(c + 1) * LANES] * scale, NEG_BIG))
        m = jnp.max(functools.reduce(jnp.maximum, ss), axis=-1, keepdims=True)
        ps = [jnp.where(ok, jnp.exp(s - m), 0.0) for ok, s in zip(oks, ss)]
        l = jnp.sum(functools.reduce(jnp.add, ps), axis=-1, keepdims=True)
        p = jnp.concatenate(ps, axis=1).astype(BF)
        o = jnp.dot(p, vb[g * span:(g + 1) * span, :], preferred_element_type=F32)
        stat = jnp.zeros((gr, LANES), F32)
        for h in range(heads):
            hs = slice(h * gr, (h + 1) * gr)
            part_b[rs, h * hd:(h + 1) * hd] = o[hs]
            stat = jnp.where(lane == h, m[hs], stat)
            stat = jnp.where(lane == heads + h, l[hs], stat)
        part_b[rs, qw:] = stat
    k_out.wait()
    v_out.wait()


def self_phase(pos, hid, gain, wq, wk, wv, ks, vs, *, scale):
    rows, hidden = hid.shape
    tlen = ks.shape[1]
    hd = ks.shape[2]
    heads = wq.shape[1] // hd
    chunks = 4
    ks = ks.reshape(rows * tlen, hd)
    vs = vs.reshape(rows * tlen, hd)
    freq = rope_table(hd)
    anys = pl.BlockSpec(memory_space=pl.ANY)
    cache = jax.ShapeDtypeStruct(ks.shape, BF)
    pshape = (rows, heads * hd + LANES)
    return pl.pallas_call(
        functools.partial(self_kernel, chunks=chunks, heads=heads, scale=scale),
        out_shape=(jax.ShapeDtypeStruct(pshape, F32), cache, cache),
        in_specs=[pl.BlockSpec(memory_space=pltpu.SMEM)] + [anys] * 8,
        out_specs=(pl.BlockSpec(memory_space=pltpu.VMEM), anys, anys),
        scratch_shapes=[
            pltpu.VMEM(freq.shape, F32), pltpu.VMEM((rows, hidden), BF), pltpu.VMEM(gain.shape, BF),
            pltpu.VMEM((rows, hidden), BF), pltpu.VMEM(wq.shape, BF),
            pltpu.VMEM(wk.shape, BF), pltpu.VMEM(wv.shape, BF),
            pltpu.VMEM(ks.shape, BF), pltpu.VMEM(vs.shape, BF),
            pltpu.VMEM((heads, rows, hd), F32), pltpu.VMEM((rows, hd), F32), pltpu.VMEM((rows, hd), F32),
            pltpu.VMEM((rows, LANES), jnp.int32),
            pltpu.VMEM((rows // GROUP_ROWS, heads * GROUP_ROWS, GROUP_ROWS * tlen), F32),
            pltpu.SemaphoreType.DMA((5,)), pltpu.SemaphoreType.DMA((chunks,)), pltpu.SemaphoreType.DMA((2,)),
            pltpu.SemaphoreType.DMA((2,)),
        ],
        compiler_params=pltpu.CompilerParams(vmem_limit_bytes=60 << 20),
        name="self_attention",
    )(pos, freq, hid, gain, wq, wk, wv, ks, vs)


def step_kernel(mask_sm, gate_sm, part_b, g2_hbm, g3_hbm, g4_hbm, qn_hbm, xv_hbm,
                hid_hbm, wo_hbm, wg_hbm, wu_hbm, wd_hbm, wqc_hbm, woc_hbm, wgc_hbm, wuc_hbm, wdc_hbm, kc_hbm, vc_hbm,
                out_ref,
                wo_b, chunk_b, qc_b, down_b, kc_b, vc_b, hid_b, comb, sbuf, rbuf, piece, full, stat, stats, acc_s, act, ob,
                fin, gain_b, gain_f, qn_ref, xv_ref, small_sem,
                wo_sem, chunk_sem, qc_sem, down_sem, kv_sem, hid_sem, cs_sem, cr_sem, rs_ssem, rs_rsem, ag_ssem, ag_rsem,
                st_ssem, st_rsem, fd_ssem, fd_rsem, ff_ssem, ff_rsem, fc_ssem, fc_rsem, *, n_sp, n_tp, heads, scale):
    sp = lax.axis_index("sp")
    tp = lax.axis_index("tp")
    xx = tp // 2
    cc = tp % 2
    n_x = n_tp // 2
    rows = hid_b.shape[0]
    wide = hid_b.shape[1]
    mlp = act.shape[1]
    hd = LANES
    gr = GROUP_ROWS
    per = wide // LANES
    r0 = pl.multiple_of(sp * rows, rows)

    def tp_at(k):
        dx, dc = ORDER[k]
        return ((xx + dx) % n_x) * 2 + (cc + dc) % 2

    def remote(src, dst, ssem, rsem, **dev):
        return pltpu.make_async_remote_copy(src_ref=src, dst_ref=dst, send_sem=ssem, recv_sem=rsem,
                                            device_id=dev, device_id_type=MESH)

    bar = pltpu.get_barrier_semaphore()
    for j in range(1, n_sp):
        pl.semaphore_signal(bar, inc=1, device_id={"sp": (sp + j) % n_sp}, device_id_type=MESH)
    for k in range(1, n_tp):
        pl.semaphore_signal(bar, inc=1, device_id={"tp": tp_at(k)}, device_id_type=MESH)

    def chunk_copies(n):
        slot = n % CHUNK_SLOTS
        a, b = ((wg_hbm, wu_hbm), (wgc_hbm, wuc_hbm))[n // n_tp]
        src = pl.ds(pl.multiple_of(tp_at(n % n_tp) * wide, wide), wide)
        return [pltpu.make_async_copy(a.at[src], chunk_b.at[slot, :, pl.ds(0, mlp)], chunk_sem.at[slot, 0]),
                pltpu.make_async_copy(b.at[src], chunk_b.at[slot, :, pl.ds(mlp, mlp)], chunk_sem.at[slot, 1])]

    def start_chunks(first, last):
        for n in range(first, last):
            for cp in chunk_copies(n):
                cp.start()

    def chip_at(i):
        return (xx + CHIPS[i]) % n_x

    def down_copy(layer, i):
        src = (wd_hbm, wdc_hbm)[layer]
        return pltpu.make_async_copy(src.at[:, pl.ds(pl.multiple_of(chip_at(i) * 2 * wide, LANES), 2 * wide)],
                                     down_b.at[i], down_sem.at[i])

    def load_down(layer):
        for i in range(n_x):
            down_copy(layer, i).start()

    wo_copy = pltpu.make_async_copy(wo_hbm, wo_b, wo_sem)
    woc_copy = pltpu.make_async_copy(woc_hbm, wo_b, wo_sem)
    qc_copy = pltpu.make_async_copy(wqc_hbm, qc_b, qc_sem)
    hid_copy = pltpu.make_async_copy(
        hid_hbm.at[pl.ds(r0, rows), pl.ds(pl.multiple_of(tp * wide, LANES), wide)], hid_b, hid_sem)
    kc_copy = pltpu.make_async_copy(kc_hbm.at[pl.ds(r0, rows)], kc_b, kv_sem.at[0])
    vc_copy = pltpu.make_async_copy(vc_hbm.at[pl.ds(r0, rows)], vc_b, kv_sem.at[1])
    small = [pltpu.make_async_copy(g2_hbm, gain_b.at[0], small_sem.at[1]),
             pltpu.make_async_copy(g3_hbm, gain_b.at[1], small_sem.at[2]),
             pltpu.make_async_copy(g4_hbm, gain_b.at[2], small_sem.at[3]),
             pltpu.make_async_copy(qn_hbm, qn_ref, small_sem.at[4]),
             pltpu.make_async_copy(xv_hbm.at[pl.ds(r0, rows)], xv_ref, small_sem.at[5])]
    for cp in small:
        cp.start()
    wo_copy.start()
    hid_copy.start()
    start_chunks(0, 3)
    pl.semaphore_wait(bar, n_sp - 1 + n_tp - 1)

    sends = []
    for i, j in enumerate((2, 1, 3)):
        peer = (sp + j) % n_sp
        cp = remote(part_b.at[pl.ds(pl.multiple_of(peer * rows, rows), rows)], comb.at[i],
                    cs_sem.at[i], cr_sem.at[i], sp=peer)
        cp.start()
        sends.append(cp)
    start_chunks(3, CHUNK_SLOTS)
    for cp in small:
        cp.wait()
    for i in range(3):
        g_all = gain_b[i].astype(F32)
        for j in range(n_tp):
            gain_f[i, j] = g_all[j * per:(j + 1) * per, :]
    for cp in sends:
        cp.wait()
    load_down(0)
    qw = heads * hd
    own = part_b[pl.ds(r0, rows), :]
    blocks = [own] + [comb[j] for j in range(n_sp - 1)]
    for h in range(heads):
        ms = [b[:, qw + h:qw + h + 1] for b in blocks]
        top = functools.reduce(jnp.maximum, ms)
        fs = [jnp.exp(m - top) for m in ms]
        den = sum(b[:, qw + heads + h:qw + heads + h + 1] * f for b, f in zip(blocks, fs))
        num = sum(b[:, h * hd:(h + 1) * hd] * f for b, f in zip(blocks, fs))
        ob[:, h * hd:(h + 1) * hd] = (num / den).astype(BF)

    whole = ((0, 0, rows),)
    halves = ((0, 0, rows // 2), (1, rows // 2, rows // 2))
    last = 2 * (n_x - 1)

    def reduce_send(product, parts):
        sent = []
        for i in range(n_x):
            out = product(i)
            lo = parts[0][1]
            n = out.shape[0]
            sbuf[2 * i, lo:lo + n] = out[:, :wide]
            sbuf[2 * i + 1, lo:lo + n] = out[:, wide:]
            if i < n_x - 1:
                for h, r, n in parts:
                    for c in range(2):
                        cp = remote(sbuf.at[2 * i + c, pl.ds(r, n)], rbuf.at[2 * i + cc, pl.ds(r, n)],
                                    rs_ssem.at[h, 2 * i + c], rs_rsem.at[h, 2 * i + cc], tp=chip_at(i) * 2 + c)
                        cp.start()
                        sent.append(cp)
        for h, r, n in parts:
            cp = remote(sbuf.at[last + 1 - cc, pl.ds(r, n)], rbuf.at[last, pl.ds(r, n)], rs_ssem.at[h, last],
                        rs_rsem.at[h, last], tp=xx * 2 + 1 - cc)
            cp.start()
            sent.append(cp)
        return sent

    def reduce_wait(part):
        h, r, n = part
        acc = sbuf[last + cc, r:r + n]
        for j in (6, 2, 3, 4, 5, 0, 1):
            remote(sbuf.at[j, pl.ds(r, n)], rbuf.at[j, pl.ds(r, n)], rs_ssem.at[h, j], rs_rsem.at[h, j],
                   tp=xx * 2 + 1 - cc).wait_recv()
            acc = acc + rbuf[j, r:r + n]
        return acc

    def done(sent):
        for cp in sent:
            cp.wait_send()

    def reduce_scatter(product, then=None):
        sent = reduce_send(product, whole)
        if then is not None:
            then()
        acc = reduce_wait(whole[0])
        done(sent)
        return acc

    def share_send(cur, slot, part):
        h, r, n = part
        rs = pl.ds(r, n)
        piece[slot, r:r + n] = cur
        stat[slot, r:r + n] = jnp.broadcast_to(jnp.sum(cur * cur, axis=-1, keepdims=True), (n, LANES))
        sent = []
        for k in range(1, n_tp):
            cp = remote(stat.at[slot, rs], stats.at[k - 1, rs], st_ssem.at[h, k - 1], st_rsem.at[h, k - 1], tp=tp_at(k))
            cp.start()
            sent.append(cp)
        for k in range(1, n_tp):
            cp = remote(piece.at[slot, rs], full.at[k - 1, rs], ag_ssem.at[h, k - 1], ag_rsem.at[h, k - 1], tp=tp_at(k))
            cp.start()
            sent.append(cp)
        return sent

    def share_use(cur, slot, part, gain, use):
        h, r, n = part
        rs = pl.ds(r, n)
        tot = stat[slot, r:r + n]
        for k in range(1, n_tp):
            remote(stat.at[slot, rs], stats.at[k - 1, rs], st_ssem.at[h, k - 1], st_rsem.at[h, k - 1],
                   tp=tp_at(k)).wait_recv()
            tot = tot + stats[k - 1, r:r + n]
        inv = lax.rsqrt(tot * (1.0 / (n_tp * wide)) + NORM_EPS)
        for k in range(n_tp):
            if k == 0:
                v = cur
            else:
                j = FROM[k] - 1
                remote(piece.at[slot, rs], full.at[j, rs], ag_ssem.at[h, j], ag_rsem.at[h, j], tp=tp_at(k)).wait_recv()
                v = full[j, r:r + n]
            g = gain_f[gain, tp_at(k)]
            x = [v[:, i * LANES:(i + 1) * LANES] * inv * g[i:i + 1, :] for i in range(per)]
            use(k, jnp.concatenate(x, axis=1).astype(BF))

    def gate_up(layer, cur, slot, gain):
        def use(k, x):
            n = layer * n_tp + k
            for cp in chunk_copies(n):
                cp.wait()
            out = jnp.dot(x, chunk_b[n % CHUNK_SLOTS], preferred_element_type=F32)
            if k == 0:
                acc_s[...] = out
            else:
                acc_s[...] += out
            if k + CHUNK_SLOTS < n_tp:
                start_chunks(n + CHUNK_SLOTS, n + CHUNK_SLOTS + 1)

        sent = share_send(cur, slot, whole[0])
        share_use(cur, slot, whole[0], gain, use)
        done(sent)
        gate = acc_s[:, :mlp].astype(BF).astype(F32)
        up = acc_s[:, mlp:].astype(BF).astype(F32)
        act[...] = (gate * jax.nn.sigmoid(gate) * up).astype(BF)

    def load_cross_mlp():
        start_chunks(n_tp, n_tp + CHUNK_SLOTS)
        load_down(1)

    def down(layer):
        def product(i):
            down_copy(layer, i).wait()
            return jnp.dot(act[...], down_b[i], preferred_element_type=F32)

        return product

    def wo_product(i, r=0, n=rows):
        return jnp.dot(ob[r:r + n, :], wo_b[:, pl.ds(pl.multiple_of(chip_at(i) * 2 * wide, LANES), 2 * wide)],
                       preferred_element_type=F32)

    def rounded(v):
        return v.astype(BF).astype(F32)

    def row_scale(i):
        sub = lax.broadcasted_iota(jnp.int32, (rows, LANES), 0)
        out = jnp.zeros((rows, LANES), jnp.int32)
        for r in range(rows):
            out = jnp.where(sub == r, mask_sm[r0 + r], out)
        return (jnp.tanh(jnp.full((rows, LANES), gate_sm[i], F32)) * out.astype(F32))[:, 0:1]

    wo_copy.wait()
    acc = reduce_scatter(wo_product)
    hid_copy.wait()
    gate_up(0, rounded(hid_b[...].astype(F32) + acc), 0, 0)
    woc_copy.start()
    qc_copy.start()
    kc_copy.start()
    vc_copy.start()
    sent_d = reduce_send(down(0), halves)
    load_cross_mlp()

    cur, sent_g = [], []
    for part in halves:
        h, r, n = part
        cur.append(rounded(piece[0, r:r + n] + reduce_wait(part)))
        sent_g += share_send(cur[h], 1, part)
    done(sent_d)
    qc_copy.wait()
    kc_copy.wait()
    vc_copy.wait()
    woc_copy.wait()
    n_vis = kc_b.shape[1]
    rmod = lax.broadcasted_iota(jnp.int32, (heads * gr, n_vis), 0) % gr
    sent_o = []
    for part in halves:
        g, r, _ = part
        q_parts = []

        def use_q(k, x):
            w = qc_b[pl.ds(pl.multiple_of(tp_at(k) * wide, wide), wide), :]
            out = jnp.dot(x, w, preferred_element_type=F32)
            q_parts[:] = [out if k == 0 else q_parts[0] + out]

        share_use(cur[g], 1, part, 1, use_q)
        qs = []
        for h in range(heads):
            v = rounded(q_parts[0][:, h * hd:(h + 1) * hd])
            inv = lax.rsqrt(jnp.mean(v * v, axis=-1, keepdims=True) + NORM_EPS)
            qs.append(rounded(v * inv * qn_ref[...].astype(F32)))
        qg = jnp.concatenate(qs, axis=0).astype(BF)
        s = jnp.zeros((heads * gr, n_vis), F32)
        for i in range(gr):
            s_i = lax.dot_general(qg, kc_b[r + i], NT_DIMS, preferred_element_type=F32)
            s = jnp.where(rmod == i, s_i, s)
        valid = xv_ref[r:r + gr, :]
        ok = jnp.concatenate([valid] * heads, axis=0) > 0
        s = jnp.where(ok, s * scale, NEG_BIG)
        m = jnp.max(s, axis=-1, keepdims=True)
        pr = jnp.where(ok, jnp.exp(s - m), 0.0)
        l = jnp.sum(pr, axis=-1, keepdims=True)
        o = jnp.zeros((heads * gr, hd), F32)
        for i in range(gr):
            o = o + jnp.dot(jnp.where(rmod == i, pr, 0.0).astype(BF), vc_b[r + i], preferred_element_type=F32)
        o = o / l
        for h in range(heads):
            ob[r:r + gr, h * hd:(h + 1) * hd] = o[h * gr:(h + 1) * gr].astype(BF)
        sent_o += reduce_send(functools.partial(wo_product, r=r, n=gr), (part,))
    done(sent_g)
    acc = jnp.concatenate([reduce_wait(part) for part in halves], axis=0)
    done(sent_o)

    gate_up(1, rounded(piece[1] + row_scale(0) * acc), 0, 2)
    acc = reduce_scatter(down(1))
    fin[cc, sp, xx] = rounded(piece[0] + row_scale(1) * acc)

    half = rows // 2
    top = pl.ds(0, half)
    bot = pl.ds(half, half)

    def hop_x(src_sp, src_x, part, dx, ssem, rsem):
        blk = fin.at[cc, src_sp, src_x, part]
        return remote(blk, blk, ssem, rsem, tp=((xx + dx) % n_x) * 2 + cc)

    def hop_y(src_sp, src_x, part, dy, ssem, rsem):
        blk = fin.at[cc, src_sp, src_x, part]
        return remote(blk, blk, ssem, rsem, sp=(sp + dy) % n_sp)

    across = []

    def hop_core(src_sp, src_x, *part):
        blk = fin.at[(cc, src_sp, src_x) + part]
        i = len(across)
        cp = remote(blk, blk, fc_ssem.at[i], fc_rsem.at[i], tp=xx * 2 + (1 - cc))
        cp.start()
        across.append(cp)

    steps = (1, 3, 2)
    first = []
    for i, d in enumerate(steps):
        cx = hop_x(sp, xx, top, d, fd_ssem.at[0, i], fd_rsem.at[0, i])
        cy = hop_y(sp, xx, bot, d, fd_ssem.at[1, i], fd_rsem.at[1, i])
        cx.start()
        cy.start()
        first.append((cx, cy))
    second = []

    def forward(a, from_x, from_y):
        for i, d in enumerate(steps):
            cy = hop_y(sp, from_x, top, d, ff_ssem.at[0, a, i], ff_rsem.at[0, a, i])
            cx = hop_x(from_y, xx, bot, d, ff_ssem.at[1, a, i], ff_rsem.at[1, a, i])
            cy.start()
            cx.start()
            second.append((cx, from_y, (xx + n_x - d) % n_x, cy, (sp + n_sp - d) % n_sp, from_x))

    forward(0, xx, sp)
    hop_core(sp, xx)
    for a, i in ((1, 0), (2, 1), (3, 2)):
        cx, cy = first[i]
        from_x = (xx + n_x - steps[i]) % n_x
        from_y = (sp + n_sp - steps[i]) % n_sp
        cx.wait_recv()
        cy.wait_recv()
        forward(a, from_x, from_y)
        hop_core(sp, from_x, top)
        hop_core(from_y, xx, bot)
    for cx, b_sp, b_x, cy, t_sp, t_x in second:
        cx.wait_recv()
        hop_core(b_sp, b_x, bot)
        cy.wait_recv()
        hop_core(t_sp, t_x, top)
    for cx, cy in first:
        cx.wait_send()
        cy.wait_send()
    for cx, _, _, cy, _, _ in second:
        cx.wait_send()
        cy.wait_send()
    for cp in across:
        cp.wait()
    for c in range(2):
        for s in range(n_sp):
            for x in range(n_x):
                j = x * 2 + c
                out_ref[s * rows:(s + 1) * rows, j * wide:(j + 1) * wide] = fin[c, s, x].astype(BF)


def step_phase(mask, gates, part, gains, qnorm, xvalid, hid, weights, kc, vc, *, n_sp, n_tp, heads, scale):
    all_rows, hidden = hid.shape
    rows = all_rows // n_sp
    wide = hidden // n_tp
    mlp = weights[1].shape[1]
    n_vis, hd = kc.shape[1], kc.shape[2]
    vm = pl.BlockSpec(memory_space=pltpu.VMEM)
    anys = pl.BlockSpec(memory_space=pl.ANY)
    dma = pltpu.SemaphoreType.DMA
    n_x = n_tp // 2
    peers = n_tp - 1
    pwide = part.shape[1]
    return pl.pallas_call(
        functools.partial(step_kernel, n_sp=n_sp, n_tp=n_tp, heads=heads, scale=scale),
        out_shape=jax.ShapeDtypeStruct((all_rows, hidden), BF),
        in_specs=[pl.BlockSpec(memory_space=pltpu.SMEM)] * 2 + [vm] + [anys] * 17,
        out_specs=vm,
        scratch_shapes=[
            pltpu.VMEM(weights[0].shape, BF),
            pltpu.VMEM((CHUNK_SLOTS, wide, 2 * mlp), BF),
            pltpu.VMEM(weights[4].shape, BF),
            pltpu.VMEM((n_x, mlp, 2 * wide), BF),
            pltpu.VMEM((rows, n_vis, hd), BF), pltpu.VMEM((rows, n_vis, hd), BF),
            pltpu.VMEM((rows, wide), BF),
            pltpu.VMEM((n_sp - 1, rows, pwide), F32),
            pltpu.VMEM((n_tp, rows, wide), F32), pltpu.VMEM((peers, rows, wide), F32),
            pltpu.VMEM((2, rows, wide), F32),
            pltpu.VMEM((peers, rows, wide), F32),
            pltpu.VMEM((2, rows, LANES), F32), pltpu.VMEM((peers, rows, LANES), F32),
            pltpu.VMEM((rows, 2 * mlp), F32),
            pltpu.VMEM((rows, mlp), BF),
            pltpu.VMEM((rows, heads * hd), BF),
            pltpu.VMEM((2, n_sp, n_x, rows, wide), F32),
            pltpu.VMEM((3,) + gains[0].shape, BF),
            pltpu.VMEM((3, n_tp, wide // LANES, LANES), F32), pltpu.VMEM(qnorm.shape, BF),
            pltpu.VMEM((rows, n_vis), jnp.int32), dma((6,)),
            dma, dma((CHUNK_SLOTS, 2)), dma, dma((n_x,)), dma((2,)), dma,
            dma((n_sp - 1,)), dma((n_sp - 1,)), dma((2, peers)), dma((2, peers)), dma((2, peers)), dma((2, peers)),
            dma((2, peers)), dma((2, peers)),
            dma((2, 3)), dma((2, 3)), dma((2, 4, 3)), dma((2, 4, 3)), dma((31,)), dma((31,)),
        ],
        compiler_params=pltpu.CompilerParams(collective_id=1, has_side_effects=True, vmem_limit_bytes=67043328),
        name="decode_step",
    )(mask, gates, part, *gains, qnorm, xvalid, hid, *weights, kc, vc)


def solution(mesh):
    cache_spec = P('dp', 'sp', 'tp', None)
    cross_spec = P('dp', None, 'tp', None)
    row_spec = P('dp', None)
    vec_spec = P('dp')
    full_spec = P(None)
    col_spec = P(None, 'tp')
    split_rows = P('tp', None)
    in_specs = (row_spec, vec_spec, cache_spec, cache_spec, cross_spec, cross_spec, row_spec, vec_spec,
                full_spec, col_spec, col_spec, col_spec, split_rows, full_spec, col_spec, col_spec, split_rows,
                full_spec, col_spec, full_spec, split_rows, full_spec, full_spec, col_spec, col_spec, split_rows)
    out_specs = (row_spec, cache_spec, cache_spec)
    n_sp = mesh.shape['sp']
    n_tp = mesh.shape['tp']

    def local_step(hidden, new_pos, k_self, v_self, k_cross, v_cross, xvalid, rowmask,
                   self_attn_norm, self_wq, self_wk, self_wv, self_wo, self_mlp_norm,
                   self_wgate, self_wup, self_wdown, cross_attn_norm, cross_wq, cross_qnorm,
                   cross_wo, cross_gates, cross_mlp_norm, cross_wgate, cross_wup, cross_wdown):
        batch_rows = hidden.shape[0]
        len_local = k_self.shape[1]
        head_dim = k_self.shape[3]
        heads = self_wq.shape[1] // head_dim
        scale = head_dim ** -0.5
        flat = (batch_rows, len_local, head_dim)
        lanes = (-1, LANES)
        part, ko, vo = self_phase(new_pos, hidden, self_attn_norm.reshape(lanes), self_wq, self_wk, self_wv,
                                  k_self.reshape(flat), v_self.reshape(flat), scale=scale)
        gains = tuple(g.reshape(lanes) for g in (self_mlp_norm, cross_attn_norm, cross_mlp_norm))
        weights = (self_wo, self_wgate, self_wup, self_wdown, cross_wq, cross_wo, cross_wgate, cross_wup, cross_wdown)
        cflat = (batch_rows, k_cross.shape[1], head_dim)
        h4 = step_phase(rowmask, cross_gates, part, gains, cross_qnorm.reshape(lanes), xvalid,
                        hidden, weights, k_cross.reshape(cflat), v_cross.reshape(cflat),
                        n_sp=n_sp, n_tp=n_tp, heads=heads, scale=scale)
        return h4, ko.reshape(k_self.shape), vo.reshape(v_self.shape)

    return jax.shard_map(local_step, mesh=mesh, in_specs=in_specs, out_specs=out_specs, check_vma=False)
```
